32 devices in a mesh: dp: 8 (over z, y), tensor: 4 (over x, core).
Axes of the slice: x: 2, y: 2, z: 4, core: 2. Of those that a mesh axis runs over, the one named last changes fastest.
Arguments:
- tokens: bfloat16 [8704, 1024], P(('dp', 'tensor')), may hold values from -6 to 6
- text_lengths: int32 [8], P('dp'), may hold values from 1 to 64, as said below
- norm1_gain: float32 [1024], replicated, may hold values from 0.25 to 1.75
- norm1_shift: float32 [1024], replicated, may hold values from -1.75 to 1.75
- w_qkv: bfloat16 [1024, 3072], P(None, 'tensor'), may hold values from -0.25 to 0.25
- q_bias: float32 [1024], P('tensor'), may hold values from -1.75 to 1.75
- v_bias: float32 [1024], P('tensor'), may hold values from -1.75 to 1.75
- w_out: bfloat16 [1024, 1024], P('tensor'), may hold values from -1 to 1
- out_bias: float32 [1024], replicated, may hold values from -1.75 to 1.75
- norm2_gain: float32 [1024], replicated, may hold values from 0.25 to 1.75
- norm2_shift: float32 [1024], replicated, may hold values from -1.75 to 1.75
- norm3_gain: float32 [1024], replicated, may hold values from 0.25 to 1.75
- norm3_shift: float32 [1024], replicated, may hold values from -1.75 to 1.75
- w_fc1: bfloat16 [1024, 4096], P(None, 'tensor'), may hold values from -0.1875 to 0.1875
- fc1_bias: bfloat16 [4096], P('tensor'), may hold values from -3 to 3
- w_fc2: bfloat16 [4096, 1024], P('tensor'), may hold values from -0.09375 to 0.09375
- fc2_bias: float32 [1024], replicated, may hold values from -1.75 to 1.75
- norm4_gain: float32 [1024], replicated, may hold values from 0.25 to 1.75
- norm4_shift: float32 [1024], replicated, may hold values from -1.75 to 1.75
- cotangent: bfloat16 [8704, 1024], P(('dp', 'tensor')), may hold values from -16 to 16
Outputs:
- layer_out: bfloat16 [8704, 1024], P(('dp', 'tensor'))
- input_grad: float32 [8704, 1024], P(('dp', 'tensor'))
- grad_norm1_gain: float32 [1024], replicated
- grad_norm1_shift: float32 [1024], replicated
- grad_qkv: float32 [1024, 3072], P(None, 'tensor')
- grad_q_bias: float32 [1024], P('tensor')
- grad_v_bias: float32 [1024], P('tensor')
- grad_out: float32 [1024, 1024], P('tensor')
- grad_out_bias: float32 [1024], replicated
- grad_norm2_gain: float32 [1024], replicated
- grad_norm2_shift: float32 [1024], replicated
- grad_norm3_gain: float32 [1024], replicated
- grad_norm3_shift: float32 [1024], replicated
- grad_fc1: float32 [1024, 4096], P(None, 'tensor')
- grad_fc1_bias: float32 [4096], P('tensor')
- grad_fc2: float32 [4096, 1024], P('tensor')
- grad_fc2_bias: float32 [1024], replicated
- grad_norm4_gain: float32 [1024], replicated
- grad_norm4_shift: float32 [1024], replicated
The draws below stay inside these ranges and needn't reach their ends.
Inputs may be any that keep to these rules, and one draw needn't show every extreme that they name: `text_lengths`: some sequence has all 64 text positions real and some has only one.
All inputs are finite; a program needn't handle non-finite values.
Results may differ from the reference program's by a relative error of at most 0.014.
The reference program's roundings to bfloat16 on the way count: a program that leaves them out, or rounds other values in their place, can miss the bound.
Values may be sent and summed in bfloat16 or wider, within the bound.
A program may use at most 192 MiB of HBM per device.

```python
import math
import jax
import jax.numpy as jnp
from jax import lax

D = 1024
HEADS = 16
HD = 64
FF = 4096
TEXT = 64
ALPHA = 32
LEN = 1088
SEQS = 8
TOKENS = 8704


def draw_text_lengths(key, part):
    lengths = jax.random.randint(jax.random.fold_in(key, 11), (SEQS,), 1, TEXT + 1)
    ranking = jax.random.permutation(jax.random.fold_in(key, 12), SEQS)
    lengths = jnp.where(ranking == 0, TEXT, lengths)
    lengths = jnp.where(ranking == 1, 1, lengths)
    return lengths.astype(jnp.int32)


def draw_cotangent(key, part):
    seq_index = (jnp.arange(TOKENS) // LEN).astype(jnp.float32)
    rising = 0.58 * 3.0 ** (seq_index / max(SEQS - 1, 1))
    noise = jnp.clip(jax.random.normal(jax.random.fold_in(key, 23), (TOKENS, D)), -4.0, 4.0)
    return (noise * rising[:, None]).astype(jnp.bfloat16)


def level_of(own_key, extent, split, least, top_value):
    def one(axis_at, parts):
        steps = jax.random.uniform(jax.random.fold_in(jax.random.fold_in(own_key, 6), axis_at), (parts,), jnp.float32, least / len(split), top_value / len(split))
        return jnp.repeat(jnp.exp(steps), extent[axis_at] // parts).reshape((-1,) + (1,) * (len(extent) - axis_at - 1))

    factor_of = one(*split[0])
    for cut in split[1:]:
        factor_of = factor_of * one(*cut)
    return factor_of


def gaussian(own_key, shape, deviation, limit, split=(), dtype=jnp.bfloat16):
    values = jax.random.normal(own_key, shape, jnp.float32) * deviation
    if len(split) > 0:
        values = level_of(own_key, shape, split, -0.22, 0.18) * values
    return jnp.clip(values, min=-limit, max=limit).astype(dtype)


def setup_inputs(seed: int = 0) -> dict:
    arg_keys = jax.random.split(jax.random.key(seed), 21)
    tokens = gaussian(arg_keys[0], (TOKENS, D), 1.0, 6.0, ((0, 32),))
    text_lengths = draw_text_lengths(jax.random.fold_in(arg_keys[20], 71), 0)
    norm1_gain = jnp.clip(1.0 + 0.15 * jax.random.normal(arg_keys[2], (D,), jnp.float32), 0.25, 1.75)
    norm1_shift = gaussian(arg_keys[3], (D,), 0.3, 1.75, (), jnp.float32)
    w_qkv = gaussian(arg_keys[4], (D, 3 * D), (D // 2) ** -0.5, 0.25, ((1, 4),))
    q_bias = gaussian(arg_keys[5], (D,), 0.3, 1.75, ((0, 4),), jnp.float32)
    v_bias = gaussian(arg_keys[6], (D,), 0.3, 1.75, ((0, 4),), jnp.float32)
    w_out = gaussian(arg_keys[7], (D, D), (D // 32) ** -0.5, 1.0, ((0, 4),))
    out_bias = gaussian(arg_keys[8], (D,), 0.3, 1.75, (), jnp.float32)
    norm2_gain = jnp.clip(1.0 + 0.15 * jax.random.normal(arg_keys[9], (D,), jnp.float32), 0.25, 1.75)
    norm2_shift = gaussian(arg_keys[10], (D,), 0.3, 1.75, (), jnp.float32)
    norm3_gain = jnp.clip(1.0 + 0.15 * jax.random.normal(arg_keys[11], (D,), jnp.float32), 0.25, 1.75)
    norm3_shift = gaussian(arg_keys[12], (D,), 0.3, 1.75, (), jnp.float32)
    w_fc1 = gaussian(arg_keys[13], (D, FF), D ** -0.5, 0.1875, ((1, 4),))
    fc1_bias = gaussian(arg_keys[14], (FF,), 0.5, 3.0, ((0, 4),))
    w_fc2 = gaussian(arg_keys[15], (FF, D), FF ** -0.5, 0.09375, ((0, 4),))
    fc2_bias = gaussian(arg_keys[16], (D,), 0.3, 1.75, (), jnp.float32)
    norm4_gain = jnp.clip(1.0 + 0.15 * jax.random.normal(arg_keys[17], (D,), jnp.float32), 0.25, 1.75)
    norm4_shift = gaussian(arg_keys[18], (D,), 0.3, 1.75, (), jnp.float32)
    cotangent = draw_cotangent(jax.random.fold_in(arg_keys[20], 71), 0)
    return {"tokens": tokens, "text_lengths": text_lengths, "norm1_gain": norm1_gain, "norm1_shift": norm1_shift, "w_qkv": w_qkv, "q_bias": q_bias, "v_bias": v_bias, "w_out": w_out, "out_bias": out_bias, "norm2_gain": norm2_gain, "norm2_shift": norm2_shift, "norm3_gain": norm3_gain, "norm3_shift": norm3_shift, "w_fc1": w_fc1, "fc1_bias": fc1_bias, "w_fc2": w_fc2, "fc2_bias": fc2_bias, "norm4_gain": norm4_gain, "norm4_shift": norm4_shift, "cotangent": cotangent}


epsilon = 1e-05

@jax.custom_vjp
def low(v):
    return lax.optimization_barrier(v.astype(jnp.bfloat16)).astype(jnp.float32)

@jax.custom_vjp
def low_back(v):
    return v

def low_keep(v):
    return (low(v), None)

def low_pass(kept, grad):
    return (grad,)

def back_keep(v):
    return (v, None)

def back_low(kept, grad):
    return (low(grad),)
low.defvjp(low_keep, low_pass)
low_back.defvjp(back_keep, back_low)

def matmul(left, right):
    return jnp.dot(left, right, precision=lax.Precision.HIGHEST)

def layer_norm(values, norm_gain, norm_shift):
    centre = lax.optimization_barrier(jnp.mean(values, axis=-1, keepdims=True))
    centered = values - centre
    variance = lax.optimization_barrier(jnp.mean(centered * centered, axis=-1, keepdims=True))
    return centered * lax.rsqrt(variance + epsilon) * norm_gain + norm_shift

def key_valid(length):
    query_pos = lax.broadcasted_iota(jnp.int32, (LEN, LEN), 0)
    key_pos = lax.broadcasted_iota(jnp.int32, (LEN, LEN), 1)
    return (key_pos <= query_pos) & ((key_pos >= TEXT) | (key_pos < length))

def attention(query_rows, key_rows, value_rows, length):
    scores_raw = low_back(jnp.einsum('qhd,khd->hqk', query_rows, key_rows, precision=lax.Precision.HIGHEST))
    scaled = scores_raw / (ALPHA * math.sqrt(HD))
    is_valid = key_valid(length)[None]
    masked = jnp.where(is_valid, scaled, -1e+30)
    row_top = lax.optimization_barrier(jnp.max(masked, axis=-1, keepdims=True))
    exponent = jnp.where(is_valid, jnp.exp(ALPHA * (masked - row_top)), 0.0)
    weights_soft = low(exponent / lax.optimization_barrier(jnp.sum(exponent, axis=-1, keepdims=True)))
    return jnp.einsum('hqk,khd->qhd', weights_soft, value_rows, precision=lax.Precision.HIGHEST)

def layer(params, tokens_seq, length):
    norm1_gain, norm1_shift, w_qkv, q_bias, v_bias, w_out, out_bias, norm2_gain, norm2_shift, norm3_gain, norm3_shift, w_fc1, fc1_bias, w_fc2, fc2_bias, norm4_gain, norm4_shift = params
    normed_in = low(layer_norm(tokens_seq, norm1_gain, norm1_shift))
    projected = matmul(normed_in, w_qkv).reshape(LEN, HEADS, 3, HD)
    query_rows = low(low_back(projected[:, :, 0] + q_bias.reshape(HEADS, HD)))
    key_rows = low(low_back(projected[:, :, 1]))
    value_rows = low(low_back(projected[:, :, 2] + v_bias.reshape(HEADS, HD)))
    context = jax.checkpoint(attention)(query_rows, key_rows, value_rows, length)
    context = low(low_back(context.reshape(LEN, D)))
    branch = low_back(matmul(context, w_out) + out_bias)
    hidden = tokens_seq + layer_norm(branch, norm2_gain, norm2_shift)
    middle = low(layer_norm(hidden, norm3_gain, norm3_shift))
    inner_act = low_back(matmul(middle, w_fc1) + fc1_bias)
    activated = low(jax.nn.gelu(inner_act, approximate=True))
    mixed_out = low_back(matmul(activated, w_fc2) + fc2_bias)
    return hidden + layer_norm(mixed_out, norm4_gain, norm4_shift)

def reference(tokens, text_lengths, norm1_gain, norm1_shift, w_qkv, q_bias, v_bias, w_out, out_bias, norm2_gain, norm2_shift, norm3_gain, norm3_shift, w_fc1, fc1_bias, w_fc2, fc2_bias, norm4_gain, norm4_shift, cotangent):
    params = tuple((entry.astype(jnp.float32) for entry in (norm1_gain, norm1_shift, w_qkv, q_bias, v_bias, w_out, out_bias, norm2_gain, norm2_shift, norm3_gain, norm3_shift, w_fc1, fc1_bias, w_fc2, fc2_bias, norm4_gain, norm4_shift)))
    seq_tokens = tokens.astype(jnp.float32).reshape(SEQS, LEN, D)
    seq_grads = cotangent.astype(jnp.float32).reshape(SEQS, LEN, D)
    zero_grads = jax.tree.map(jnp.zeros_like, params)

    def one_sequence(totals, inputs):
        tokens_seq, grad_seq, length = inputs

        def forward(weights_all, token_rows):
            return layer(weights_all, token_rows, length)
        result, pullback = jax.vjp(forward, params, tokens_seq)
        grad_params, grad_tokens = pullback(grad_seq)
        totals = jax.tree.map(jnp.add, totals, grad_params)
        return (totals, (result.astype(jnp.bfloat16), grad_tokens))
    totals, (outputs, input_grads) = lax.scan(one_sequence, zero_grads, (seq_tokens, seq_grads, text_lengths))
    g_n1, s_n1, g_qkv, g_qb, g_vb, g_out, g_ob, g_n2, s_n2, g_n3, s_n3, g_fc1, g_b1, g_fc2, g_b2, g_n4, s_n4 = totals
    return (outputs.reshape(TOKENS, D), input_grads.reshape(TOKENS, D), g_n1, s_n1, g_qkv, g_qb, g_vb, g_out, g_ob, g_n2, s_n2, g_n3, s_n3, g_fc1, g_b1, g_fc2, g_b2, g_n4, s_n4)
```

```python
from functools import partial
import math

import jax
import jax.numpy as jnp
from jax import lax
from jax.sharding import PartitionSpec as P

HD = 64
TEXT = 64
ALPHA = 32
LEN = 1088


epsilon = 1e-05


def times_transposed(left, right):
    return lax.dot_general(
        left, right, (((1,), (1,)), ((), ())), preferred_element_type=jnp.float32
    )


def transposed_times(left, right):
    return lax.dot_general(
        left, right, (((0,), (0,)), ((), ())), preferred_element_type=jnp.float32
    )


def norm_forward(values, norm_gain, norm_shift):
    centre = jnp.mean(values, axis=-1, keepdims=True)
    centered = values - centre
    inverse = lax.rsqrt(jnp.mean(centered * centered, axis=-1, keepdims=True) + epsilon)
    normed = centered * inverse
    return (normed * norm_gain + norm_shift, normed, inverse)


def norm_backward(grad_out, normed, inverse, norm_gain):
    scaled = grad_out * norm_gain
    inner_term = (
        scaled
        - jnp.mean(scaled, axis=-1, keepdims=True)
        - normed * jnp.mean(scaled * normed, axis=-1, keepdims=True)
    )
    return (inner_term * inverse, jnp.sum(grad_out * normed, axis=0), jnp.sum(grad_out, axis=0))


def scatter_low(partial_sums):
    return lax.psum_scatter(
        partial_sums.astype(jnp.bfloat16), "tensor", scatter_dimension=0, tiled=True
    ).astype(jnp.float32)


def gelu_back(inner_act, grad_act):
    _, pullback = jax.vjp(partial(jax.nn.gelu, approximate=True), inner_act)
    return pullback(grad_act)[0]


def masked_scores(query_rows, key_rows, length):
    seq_len = query_rows.shape[0]
    scores_raw = jnp.einsum(
        "qhd,khd->hqk", query_rows, key_rows, preferred_element_type=jnp.float32
    )
    scaled = scores_raw / (ALPHA * math.sqrt(HD))
    query_pos = lax.broadcasted_iota(jnp.int32, (seq_len, seq_len), 0)
    key_pos = lax.broadcasted_iota(jnp.int32, (seq_len, seq_len), 1)
    is_valid = ((key_pos <= query_pos) & ((key_pos >= TEXT) | (key_pos < length)))[None]
    return (jnp.where(is_valid, scaled, -1e30), is_valid)


def attend_forward(inputs):
    query_rows, key_rows, value_rows, length = inputs
    masked, is_valid = masked_scores(query_rows, key_rows, length)
    row_top = jnp.max(masked, axis=-1, keepdims=True)
    exponent = jnp.where(is_valid, jnp.exp(ALPHA * (masked - row_top)), 0.0)
    row_total = jnp.sum(exponent, axis=-1, keepdims=True)
    weights_low = (exponent / row_total).astype(jnp.bfloat16)
    context = jnp.einsum(
        "hqk,khd->qhd", weights_low, value_rows, preferred_element_type=jnp.float32
    )
    return (context, row_top, row_total)


def attend_backward(inputs):
    query_rows, key_rows, value_rows, length, grad_context, row_top, row_total = inputs
    masked, is_valid = masked_scores(query_rows, key_rows, length)
    weights_soft = jnp.where(is_valid, jnp.exp(ALPHA * (masked - row_top)), 0.0) / row_total
    grad_values = jnp.einsum(
        "hqk,qhd->khd",
        weights_soft.astype(jnp.bfloat16),
        grad_context,
        preferred_element_type=jnp.float32,
    )
    grad_soft = jnp.einsum(
        "qhd,khd->hqk", grad_context, value_rows, preferred_element_type=jnp.float32
    )
    grad_expon = weights_soft * (
        grad_soft - jnp.sum(weights_soft * grad_soft, axis=-1, keepdims=True)
    )
    grad_scores = (grad_expon * ALPHA / (ALPHA * math.sqrt(HD))).astype(jnp.bfloat16)
    grad_queries = jnp.einsum(
        "hqk,khd->qhd", grad_scores, key_rows, preferred_element_type=jnp.float32
    )
    grad_keys = jnp.einsum(
        "hqk,qhd->khd", grad_scores, query_rows, preferred_element_type=jnp.float32
    )
    return (
        grad_queries.astype(jnp.bfloat16),
        grad_keys.astype(jnp.bfloat16),
        grad_values.astype(jnp.bfloat16),
    )


def local(
    tokens,
    text_lengths,
    norm1_gain,
    norm1_shift,
    w_qkv,
    q_bias,
    v_bias,
    w_out,
    out_bias,
    norm2_gain,
    norm2_shift,
    norm3_gain,
    norm3_shift,
    w_fc1,
    fc1_bias,
    w_fc2,
    fc2_bias,
    norm4_gain,
    norm4_shift,
    cotangent,
):
    seq_dev = text_lengths.shape[0]
    local_heads = q_bias.shape[0] // HD
    rows_all = seq_dev * LEN
    input_rows = tokens.astype(jnp.float32)
    first_out, first_hat, first_inv = norm_forward(input_rows, norm1_gain, norm1_shift)
    gathered_first = lax.all_gather(first_out.astype(jnp.bfloat16), "tensor", axis=0, tiled=True)
    projected = jnp.dot(gathered_first, w_qkv, preferred_element_type=jnp.float32).reshape(
        rows_all, local_heads, 3, HD
    )
    seq_shape = (seq_dev, LEN, local_heads, HD)
    query_rows = (
        (projected[:, :, 0] + q_bias.reshape(local_heads, HD))
        .astype(jnp.bfloat16)
        .reshape(seq_shape)
    )
    key_rows = projected[:, :, 1].astype(jnp.bfloat16).reshape(seq_shape)
    value_rows = (
        (projected[:, :, 2] + v_bias.reshape(local_heads, HD))
        .astype(jnp.bfloat16)
        .reshape(seq_shape)
    )
    context, row_tops, row_totals = lax.map(
        attend_forward, (query_rows, key_rows, value_rows, text_lengths)
    )
    context_low = context.reshape(rows_all, local_heads * HD).astype(jnp.bfloat16)
    branch = (
        scatter_low(jnp.dot(context_low, w_out, preferred_element_type=jnp.float32))
        + out_bias
    )
    second_out, second_hat, second_inv = norm_forward(branch, norm2_gain, norm2_shift)
    hidden = input_rows + second_out
    third_out, third_hat, third_inv = norm_forward(hidden, norm3_gain, norm3_shift)
    third_low = third_out.astype(jnp.bfloat16)
    gathered_third = lax.all_gather(third_low, "tensor", axis=0, tiled=True)
    inner_act = jnp.dot(gathered_third, w_fc1, preferred_element_type=jnp.float32) + fc1_bias
    activated = jax.nn.gelu(inner_act, approximate=True).astype(jnp.bfloat16)
    mixed_out = (
        scatter_low(jnp.dot(activated, w_fc2, preferred_element_type=jnp.float32))
        + fc2_bias
    )
    fourth_out, fourth_hat, fourth_inv = norm_forward(mixed_out, norm4_gain, norm4_shift)
    layer_out = (hidden + fourth_out).astype(jnp.bfloat16)
    grad_rows = cotangent.astype(jnp.float32)
    grad_mixed, grad_gain4, grad_shift4 = norm_backward(
        grad_rows, fourth_hat, fourth_inv, norm4_gain
    )
    mixed_low = grad_mixed.astype(jnp.bfloat16)
    grad_fc2_bias = jnp.sum(mixed_low, axis=0, dtype=jnp.float32)
    gathered_grad = lax.all_gather(mixed_low, "tensor", axis=0, tiled=True)
    grad_activated = times_transposed(gathered_grad, w_fc2)
    ffn_fc2 = transposed_times(activated, gathered_grad)
    grad_inner = gelu_back(inner_act, grad_activated).astype(jnp.bfloat16)
    ffn_fc1_bias = jnp.sum(grad_inner, axis=0, dtype=jnp.float32)
    ffn_fc1 = transposed_times(gathered_third, grad_inner)
    grad_third = scatter_low(times_transposed(grad_inner, w_fc1))
    grad_mid_norm, grad_gain3, grad_shift3 = norm_backward(
        grad_third, third_hat, third_inv, norm3_gain
    )
    grad_hidden = grad_rows + grad_mid_norm
    grad_branch, grad_gain2, grad_shift2 = norm_backward(
        grad_hidden, second_hat, second_inv, norm2_gain
    )
    branch_low = grad_branch.astype(jnp.bfloat16)
    grad_out_bias = jnp.sum(branch_low, axis=0, dtype=jnp.float32)
    gathered_branch = lax.all_gather(branch_low, "tensor", axis=0, tiled=True)
    grad_context = times_transposed(gathered_branch, w_out).astype(jnp.bfloat16).reshape(seq_shape)
    part_out = transposed_times(context_low, gathered_branch)
    grad_queries, grad_keys, grad_values = lax.map(
        attend_backward,
        (query_rows, key_rows, value_rows, text_lengths, grad_context, row_tops, row_totals),
    )
    part_q_bias = jnp.sum(grad_queries, axis=(0, 1), dtype=jnp.float32).reshape(local_heads * HD)
    part_v_bias = jnp.sum(grad_values, axis=(0, 1), dtype=jnp.float32).reshape(local_heads * HD)
    grad_projected = jnp.stack([grad_queries, grad_keys, grad_values], axis=3).reshape(
        rows_all, 3 * local_heads * HD
    )
    part_qkv = transposed_times(gathered_first, grad_projected)
    grad_first = scatter_low(times_transposed(grad_projected, w_qkv))
    grad_input_norm, grad_gain1, grad_shift1 = norm_backward(
        grad_first, first_hat, first_inv, norm1_gain
    )
    input_grad = grad_hidden + grad_input_norm
    shared = jnp.concatenate(
        [
            grad_gain1,
            grad_shift1,
            grad_gain2,
            grad_shift2,
            grad_gain3,
            grad_shift3,
            grad_gain4,
            grad_shift4,
            grad_out_bias,
            grad_fc2_bias,
        ]
    )
    owned = jnp.concatenate([part_q_bias, part_v_bias, ffn_fc1_bias])
    places = lax.axis_size("tensor")
    slots = jnp.zeros((places, owned.shape[0]), jnp.float32)
    slots = lax.dynamic_update_slice(slots, owned[None], (lax.axis_index("tensor"), 0))
    small = lax.psum(jnp.concatenate([shared, slots.reshape(-1)]), ("dp", "tensor"))
    (
        grad_gain1,
        grad_shift1,
        grad_gain2,
        grad_shift2,
        grad_gain3,
        grad_shift3,
        grad_gain4,
        grad_shift4,
        grad_out_bias,
        grad_fc2_bias,
    ) = small[: shared.shape[0]].reshape(10, -1)
    mine = lax.dynamic_slice(
        small, (shared.shape[0] + lax.axis_index("tensor") * owned.shape[0],), owned.shape
    )
    part_q_bias, part_v_bias, ffn_fc1_bias = jnp.split(
        mine, [part_q_bias.shape[0], part_q_bias.shape[0] + part_v_bias.shape[0]]
    )
    part_qkv, part_out, ffn_fc1, ffn_fc2 = (
        total.astype(jnp.float32)
        for total in lax.psum(
            tuple(part.astype(jnp.bfloat16) for part in (part_qkv, part_out, ffn_fc1, ffn_fc2)),
            "dp",
        )
    )
    return (
        layer_out,
        input_grad,
        grad_gain1,
        grad_shift1,
        part_qkv,
        part_q_bias,
        part_v_bias,
        part_out,
        grad_out_bias,
        grad_gain2,
        grad_shift2,
        grad_gain3,
        grad_shift3,
        ffn_fc1,
        ffn_fc1_bias,
        ffn_fc2,
        grad_fc2_bias,
        grad_gain4,
        grad_shift4,
    )


def solution(mesh):
    in_specs = (
        P(("dp", "tensor"), None),
        P("dp"),
        P(),
        P(),
        P(None, "tensor"),
        P("tensor"),
        P("tensor"),
        P("tensor", None),
        P(),
        P(),
        P(),
        P(),
        P(),
        P(None, "tensor"),
        P("tensor"),
        P("tensor", None),
        P(),
        P(),
        P(),
        P(("dp", "tensor"), None),
    )
    out_specs = (
        P(("dp", "tensor"), None),
        P(("dp", "tensor"), None),
        P(),
        P(),
        P(None, "tensor"),
        P("tensor"),
        P("tensor"),
        P("tensor", None),
        P(),
        P(),
        P(),
        P(),
        P(),
        P(None, "tensor"),
        P("tensor"),
        P("tensor", None),
        P(),
        P(),
        P(),
    )
    return jax.shard_map(local, mesh=mesh, in_specs=in_specs, out_specs=out_specs, check_vma=False)
```

```python
from functools import partial
import math

import jax
import jax.numpy as jnp
from jax import lax
from jax.experimental import pallas as pl
from jax.experimental.pallas import tpu as pltpu
from jax.sharding import PartitionSpec as P

HD = 64
TEXT = 64
ALPHA = 32
LEN = 1088


epsilon = 1e-05


def times_transposed(left, right):
    return lax.dot_general(
        left, right, (((1,), (1,)), ((), ())), preferred_element_type=jnp.float32
    )


def transposed_times(left, right):
    return lax.dot_general(
        left, right, (((0,), (0,)), ((), ())), preferred_element_type=jnp.float32
    )


STEP = 64
TILE = 256
MESH = pl.DeviceIdType.MESH
LOW = jnp.bfloat16


def statistics(values):
    centered = values - jnp.mean(values, axis=-1, keepdims=True)
    inverse = lax.rsqrt(jnp.mean(centered * centered, axis=-1, keepdims=True) + epsilon)
    return centered * inverse, inverse


def norm_pullback(grad, normed, inverse, gain):
    scaled = grad * gain
    return inverse * (
        scaled
        - jnp.mean(scaled, axis=-1, keepdims=True)
        - normed * jnp.mean(scaled * normed, axis=-1, keepdims=True)
    )


def before_attention(total, rows, vectors):
    (token_rows,), (gain, shift) = rows, vectors
    normed, _ = statistics(token_rows)
    return normed * gain + shift, (), ()


def after_attention(total, rows, vectors):
    (token_rows,), (bias, gain2, shift2, gain3, shift3) = rows, vectors
    branch = total + bias
    normed, _ = statistics(branch)
    hidden = token_rows + (normed * gain2 + shift2)
    third, _ = statistics(hidden)
    return third * gain3 + shift3, (branch, hidden), ()


def turn_round(total, rows, vectors):
    (hidden, grad), (bias, gain, shift) = rows, vectors
    normed, inverse = statistics(total + bias)
    layer_out = hidden + (normed * gain + shift)
    low = norm_pullback(grad, normed, inverse, gain).astype(LOW).astype(jnp.float32)
    return low, (layer_out,), (grad * normed, grad, low)


def after_feed_forward(total, rows, vectors):
    (branch, hidden, grad), (gain2, gain3) = rows, vectors
    third, inverse3 = statistics(hidden)
    grad_hidden = grad + norm_pullback(total, third, inverse3, gain3)
    second, inverse2 = statistics(branch)
    low = norm_pullback(grad_hidden, second, inverse2, gain2).astype(LOW).astype(jnp.float32)
    return low, (grad_hidden,), (total * third, total, grad_hidden * second, grad_hidden, low)


def at_the_input(total, rows, vectors):
    (token_rows, grad_hidden), (gain,) = rows, vectors
    first, inverse = statistics(token_rows)
    return None, (grad_hidden + norm_pullback(total, first, inverse, gain),), (total * first, total)


class GroupSum:
    def __init__(self, sources, results, scratch):
        self.kept, self.near, self.far = scratch[:3]
        self.sems = scratch[3:]
        self.sources, self.results = sources, results
        self.pieces = [
            (at, column)
            for at, source in enumerate(sources)
            for column in range(0, source.shape[1], TILE)
        ]
        self.half = sources[0].shape[0] // 2
        self.peers = lax.axis_size("dp") // 2
        self.part = self.half // self.peers
        group = lax.axis_index("dp")
        self.side = lax.rem(group, 2)
        self.place = lax.div(group, 2)
        self.partner = group + 1 - 2 * self.side

    def others(self):
        for hop in range(1, self.peers):
            yield (
                hop - 1,
                lax.rem(self.place + hop, self.peers),
                lax.rem(self.place + self.peers - hop, self.peers),
            )

    def device(self, place):
        return place * 2 + self.side

    def targets(self):
        return [self.partner] + [self.device(ahead) for _, ahead, _ in self.others()]

    def send(self, source, target, outgoing, incoming, device):
        return pltpu.make_async_remote_copy(
            source, target, outgoing, incoming,
            device_id={"dp": device}, device_id_type=MESH,
        )

    def rows(self, start, size):
        return pl.ds(pl.multiple_of(start, 16), size)

    def cuts(self, piece):
        at, column = self.pieces[piece]
        return self.sources[at], self.results[at], pl.ds(column, TILE), pl.ds(piece * TILE, TILE)

    def halving(self, piece):
        source, _, cut, held = self.cuts(piece)
        return self.send(
            source.at[self.rows((1 - self.side) * self.half, self.half), cut],
            self.near.at[:, held], self.sems[0].at[piece], self.sems[1].at[piece], self.partner,
        )

    def parting(self, piece, slot, ahead):
        held = pl.ds(piece * TILE, TILE)
        return self.send(
            self.kept.at[self.rows(ahead * self.part, self.part), held], self.far.at[slot, :, held],
            self.sems[2].at[slot, piece], self.sems[3].at[slot, piece], self.device(ahead),
        )

    def joining(self, piece, slot, owner, ahead):
        _, result, cut, _ = self.cuts(piece)
        region = result.at[self.rows(self.side * self.half + owner * self.part, self.part), cut]
        return self.send(
            region, region, self.sems[4].at[slot, piece], self.sems[5].at[slot, piece],
            self.device(ahead),
        )

    def doubling(self, piece, side):
        _, result, cut, _ = self.cuts(piece)
        region = result.at[self.rows(side * self.half, self.half), cut]
        return self.send(
            region, region, self.sems[6].at[piece], self.sems[7].at[piece], self.partner
        )

    def start(self):
        for piece in range(len(self.pieces)):
            self.halving(piece).start()

    def after_halving(self, piece):
        source, _, cut, held = self.cuts(piece)
        self.halving(piece).wait_recv()
        mine = source[self.rows(self.side * self.half, self.half), cut].astype(jnp.float32)
        self.kept[:, held] = (mine + self.near[:, held].astype(jnp.float32)).astype(LOW)
        for slot, ahead, _ in self.others():
            self.parting(piece, slot, ahead).start()

    def after_parting(self, piece):
        _, result, cut, held = self.cuts(piece)
        total = self.kept[self.rows(self.place * self.part, self.part), held].astype(jnp.float32)
        for slot, ahead, _ in self.others():
            self.parting(piece, slot, ahead).wait_recv()
            total = total + self.far[slot, :, held].astype(jnp.float32)
        own = self.rows(self.side * self.half + self.place * self.part, self.part)
        result[own, cut] = total.astype(LOW)
        for slot, ahead, _ in self.others():
            self.joining(piece, slot, self.place, ahead).start()

    def after_joining(self, piece):
        for slot, ahead, behind in self.others():
            self.joining(piece, slot, behind, ahead).wait_recv()
        self.doubling(piece, self.side).start()

    def settle(self, piece):
        self.doubling(piece, 1 - self.side).wait_recv()
        self.doubling(piece, self.side).wait_send()
        self.halving(piece).wait_send()
        for slot, ahead, _ in self.others():
            self.parting(piece, slot, ahead).wait_send()
            self.joining(piece, slot, self.place, ahead).wait_send()


def group_sum_scratch(sources):
    pieces = sum(source.shape[1] for source in sources) // TILE
    half = sources[0].shape[0] // 2
    peers = lax.axis_size("dp") // 2
    width = pieces * TILE
    pair, fan = pltpu.SemaphoreType.DMA((pieces,)), pltpu.SemaphoreType.DMA((peers - 1, pieces))
    return [
        pltpu.VMEM((half, width), LOW),
        pltpu.VMEM((half, width), LOW),
        pltpu.VMEM((peers - 1, half // peers, width), LOW),
    ] + [pair, pair, fan, fan, fan, fan, pair, pair]


class SmallSum:
    def __init__(self, shared, owned, fresh, shared_out, owned_out, part, parts, turn, turns, last,
                 lasts, part_out, part_in, turn_out, turn_in, last_out, last_in):
        self.shared, self.owned, self.fresh = shared, owned, fresh
        self.shared_out, self.owned_out = shared_out, owned_out
        self.part, self.parts, self.turn, self.turns = part, parts, turn, turns
        self.last, self.lasts = last, lasts
        self.sems = part_out, part_in, turn_out, turn_in, last_out, last_in
        self.places, groups = lax.axis_size("tensor"), lax.axis_size("dp")
        self.groups = groups
        self.me, self.group = lax.axis_index("tensor"), lax.axis_index("dp")
        self.peers = [lax.rem(self.me + hop, self.places) for hop in range(1, self.places)]
        self.others = [lax.rem(self.group + hop, groups) for hop in range(1, groups)]
        self.n_fresh = fresh.shape[0]
        self.n_shared = self.n_fresh + shared.shape[0]
        self.quarter = shared.shape[-1] // self.places

    def sends(self, stage):
        axis = "dp" if stage == 1 else "tensor"
        outgoing, incoming = self.sems[2 * stage], self.sems[2 * stage + 1]
        for hop, peer in enumerate(self.others if stage == 1 else self.peers):
            if stage == 0:
                source, target = self.part.at[peer], self.parts.at[hop]
            elif stage == 1:
                source, target = self.turn, self.turns.at[self.group]
            else:
                source, target = self.last, self.lasts.at[self.me]
            yield pltpu.make_async_remote_copy(
                source, target, outgoing.at[hop], incoming.at[hop],
                device_id={axis: peer}, device_id_type=MESH,
            )

    def first_send(self):
        for place in range(self.places):
            cut = slice(place * self.quarter, (place + 1) * self.quarter)
            self.part[place, : self.n_fresh] = jnp.sum(self.fresh[:, :, cut], axis=1)
            self.part[place, self.n_fresh :] = jnp.sum(self.shared[:, :, cut], axis=1)
        for send in self.sends(0):
            send.start()

    def first_wait(self):
        total = self.part[self.me]
        for hop, send in enumerate(self.sends(0)):
            send.wait()
            total = total + self.parts[hop]
        self.turn[: self.n_shared] = total
        self.turn[self.n_shared :] = self.owned[...]
        self.turns[self.group] = self.turn[...]

    def second_send(self):
        for send in self.sends(1):
            send.start()

    def second_wait(self):
        for send in self.sends(1):
            send.wait()
        total = self.turns[0]
        for at in range(1, self.groups):
            total = total + self.turns[at]
        self.owned_out[...] = total[self.n_shared :]
        self.last[...] = total[: self.n_shared]
        self.lasts[self.me] = total[: self.n_shared]

    def third_send(self):
        for send in self.sends(2):
            send.start()

    def third_wait(self):
        for send in self.sends(2):
            send.wait()
        for place in range(self.places):
            cut = slice(place * self.quarter, (place + 1) * self.quarter)
            self.shared_out[:, cut] = self.lasts[place]


def small_sum_scratch(n_shared, owned):
    places, groups = lax.axis_size("tensor"), lax.axis_size("dp")
    quarter = owned.shape[1]
    depth = n_shared + owned.shape[0]
    return [
        pltpu.VMEM((places, n_shared, quarter), jnp.float32),
        pltpu.VMEM((places - 1, n_shared, quarter), jnp.float32),
        pltpu.VMEM((depth, quarter), jnp.float32),
        pltpu.VMEM((groups, depth, quarter), jnp.float32),
        pltpu.VMEM((n_shared, quarter), jnp.float32),
        pltpu.VMEM((places, n_shared, quarter), jnp.float32),
    ] + [
        pltpu.SemaphoreType.DMA((count,))
        for count in (places - 1, places - 1, groups - 1, groups - 1, places - 1, places - 1)
    ]


def segment_kernel(middle, counts, flipped, sending, *refs):
    n_rows, n_vectors, n_outs, n_sums, n_grouped = counts
    refs = list(refs)

    def take(count):
        taken = refs[:count]
        del refs[:count]
        return taken

    summing = flipped is not None
    if summing:
        left, right = take(2)
    row_refs, vector_refs = take(n_rows), take(n_vectors)
    if n_grouped:
        group_sources = take(n_grouped)
        small_in = take(2)
    gathered = take(1)[0] if sending else None
    out_refs = take(n_outs)
    if n_grouped:
        group_results = take(n_grouped)
        small_out = take(2)
    sums = take(1)[0] if n_sums else None
    if summing:
        give, got, keep, onward, came, give_sem, got_sem, out_sem, in_sem = take(9)
    if sending:
        near_out, near_in, far_out, far_in, on_out, on_in = take(6)
    if n_grouped:
        grouped = GroupSum(group_sources, group_results, take(11))
        small = SmallSum(*small_in, sums, *small_out, *take(12))

    me = lax.axis_index("tensor")
    partner = me + 1 - 2 * lax.rem(me, 2)
    across = lax.rem(me + 2, 4)
    diagonal = 3 - me
    share, width = row_refs[0].shape
    whole = share // STEP
    rest = share - whole * STEP

    def each(body):
        def one(at, carry):
            body(at, pl.multiple_of(at * STEP, STEP), STEP)
            return carry

        lax.fori_loop(0, whole, one, 0)
        if rest:
            body(whole, whole * STEP, rest)

    barrier = pltpu.get_barrier_semaphore()
    for peer in (partner, across):
        pl.semaphore_signal(barrier, inc=1, device_id={"tensor": peer}, device_id_type=MESH)
    if n_grouped:
        pl.semaphore_signal(
            barrier, inc=1, device_id={"tensor": diagonal}, device_id_type=MESH
        )
        for other in small.others:
            pl.semaphore_signal(barrier, inc=1, device_id={"dp": other}, device_id_type=MESH)
        pl.semaphore_wait(barrier, 3 + len(small.others))
        grouped.start()
    else:
        pl.semaphore_wait(barrier, 2)

    def product(block, target):
        rows = pl.ds(pl.multiple_of(block * share, 16), share)

        def one(at, carry):
            cut = pl.ds(pl.multiple_of(at * TILE, TILE), TILE)
            if flipped:
                value = times_transposed(left[rows, :], right[cut, :])
            else:
                value = jnp.dot(left[rows, :], right[:, cut], preferred_element_type=jnp.float32)
            target[:, cut] = value.astype(target.dtype)
            return carry

        lax.fori_loop(0, width // TILE, one, 0)

    if summing:

        def gift(at):
            return pltpu.make_async_remote_copy(
                give.at[at], got.at[at], give_sem.at[at], got_sem.at[at],
                device_id={"tensor": partner}, device_id_type=MESH,
            )

        def crossing(at, start, size):
            cut = pl.ds(start, size)
            return pltpu.make_async_remote_copy(
                onward.at[cut], came.at[cut], out_sem.at[at], in_sem.at[at],
                device_id={"tensor": across}, device_id_type=MESH,
            )

        product(diagonal, give.at[0])
        product(across, keep.at[0])
        gift(0).start()
        product(partner, give.at[1])
        gift(0).wait_recv()

        def pass_on(at, start, size):
            cut = pl.ds(start, size)
            onward[cut] = (keep[0, cut] + got[0, cut].astype(jnp.float32)).astype(LOW)
            crossing(at, start, size).start()

        each(pass_on)
        gift(1).start()
        product(me, keep.at[1])
        gift(1).wait_recv()

    if n_sums:
        sums[...] = jnp.zeros_like(sums)
    vectors = [ref[...] for ref in vector_refs]

    def spread(target, block, sems, at, start, size):
        cut = pl.ds(pl.multiple_of(block * share + start, 16), size)
        return pltpu.make_async_remote_copy(
            gathered.at[cut], gathered.at[cut], sems[0].at[at], sems[1].at[at],
            device_id={"tensor": target}, device_id_type=MESH,
        )

    def finish(at, start, size):
        cut = pl.ds(start, size)
        total = None
        if summing:
            crossing(at, start, size).wait_recv()
            total = (
                keep[1, cut] + got[1, cut].astype(jnp.float32) + came[cut].astype(jnp.float32)
            )
        result, outs, terms = middle(
            total, [ref[cut].astype(jnp.float32) for ref in row_refs], vectors
        )
        if sending:
            own = pl.ds(pl.multiple_of(me * share + start, 16), size)
            gathered[own] = result.astype(LOW)
        for ref, value in zip(out_refs, outs):
            ref[cut] = value.astype(ref.dtype)
        for index, term in enumerate(terms):
            sums[index] += jnp.sum(term.reshape(size // 8, 8, width), axis=0)
        if sending:
            spread(across, me, (far_out, far_in), at, start, size).start()
            spread(partner, me, (near_out, near_in), at, start, size).start()

    if n_grouped:
        pieces = len(grouped.pieces)
        early = pieces // 2
        for piece in range(early):
            grouped.after_halving(piece)
        each(finish)
        small.first_send()
        for piece in range(early, pieces):
            grouped.after_halving(piece)
            grouped.after_parting(piece - early)
        small.first_wait()
        small.second_send()
        for piece in range(pieces - early, pieces):
            grouped.after_joining(piece - (pieces - early))
            grouped.after_parting(piece)
        small.second_wait()
        small.third_send()
        for piece in range(early, pieces):
            grouped.after_joining(piece)
        small.third_wait()
        for piece in range(pieces):
            grouped.settle(piece)
    else:
        each(finish)

    if sending:

        def relay(at, start, size):
            spread(across, across, (far_out, far_in), at, start, size).wait_recv()
            spread(partner, across, (on_out, on_in), at, start, size).start()

        def settle(at, start, size):
            spread(partner, partner, (near_out, near_in), at, start, size).wait()
            spread(across, me, (far_out, far_in), at, start, size).wait_send()
            spread(partner, diagonal, (on_out, on_in), at, start, size).wait()

        each(relay)
        each(settle)
    if summing:
        gift(0).wait_send()
        gift(1).wait_send()
        each(lambda at, start, size: crossing(at, start, size).wait_send())


def segment(number, middle, rows, vectors, outs, n_sums, product=None, sending=True,
            grouped=None):
    share, width = rows[0].shape
    flipped = None
    operands = []
    shapes = []
    scratch = []
    pieces = -(-share // STEP)
    places = lax.axis_size("tensor")
    flops = 0
    if product is not None:
        left, right, flipped = product
        operands += [left, right]
        flops = 2 * left.shape[0] * right.size
        scratch += [
            pltpu.VMEM((2, share, width), LOW),
            pltpu.VMEM((2, share, width), LOW),
            pltpu.VMEM((2, share, width), jnp.float32),
            pltpu.VMEM((share, width), LOW),
            pltpu.VMEM((share, width), LOW),
            pltpu.SemaphoreType.DMA((2,)),
            pltpu.SemaphoreType.DMA((2,)),
            pltpu.SemaphoreType.DMA((pieces,)),
            pltpu.SemaphoreType.DMA((pieces,)),
        ]
    operands += list(rows) + [vector.reshape(1, width) for vector in vectors]
    n_grouped = 0
    if grouped is not None:
        sources, small_shared, small_owned = grouped
        n_grouped = len(sources)
        n_shared = n_sums + small_shared.shape[0]
        operands += list(sources) + [small_shared, small_owned]
    if sending:
        shapes.append(jax.ShapeDtypeStruct((places * share, width), LOW))
        scratch += [pltpu.SemaphoreType.DMA((pieces,))] * 6
    shapes += [jax.ShapeDtypeStruct((share, width), dtype) for dtype in outs]
    if n_grouped:
        shapes += [jax.ShapeDtypeStruct(source.shape, LOW) for source in sources]
        shapes.append(jax.ShapeDtypeStruct((n_shared, width), jnp.float32))
        shapes.append(jax.ShapeDtypeStruct(small_owned.shape, jnp.float32))
        scratch += group_sum_scratch(sources) + small_sum_scratch(n_shared, small_owned)
    if n_sums:
        shapes.append(jax.ShapeDtypeStruct((n_sums, 8, width), jnp.float32))
    counts = (len(rows), len(vectors), len(outs), n_sums, n_grouped)
    in_vmem = pl.BlockSpec(memory_space=pltpu.VMEM)
    moved = sum(item.size * item.dtype.itemsize for item in operands + shapes)
    return pl.pallas_call(
        partial(segment_kernel, middle, counts, flipped, sending),
        out_shape=shapes,
        in_specs=[in_vmem] * len(operands),
        out_specs=[in_vmem] * len(shapes),
        scratch_shapes=scratch,
        compiler_params=pltpu.CompilerParams(
            collective_id=number, has_side_effects=True, vmem_limit_bytes=48 * 2**20
        ),
        cost_estimate=pl.CostEstimate(
            flops=flops + 25_000_000_000, bytes_accessed=moved, transcendentals=0
        ),
    )(*operands)


def gelu_back(inner_act, grad_act):
    _, pullback = jax.vjp(partial(jax.nn.gelu, approximate=True), inner_act)
    return pullback(grad_act)[0]


def masked_scores(query_rows, key_rows, length):
    seq_len = query_rows.shape[0]
    scores_raw = jnp.einsum(
        "qhd,khd->hqk", query_rows, key_rows, preferred_element_type=jnp.float32
    )
    scaled = scores_raw / (ALPHA * math.sqrt(HD))
    query_pos = lax.broadcasted_iota(jnp.int32, (seq_len, seq_len), 0)
    key_pos = lax.broadcasted_iota(jnp.int32, (seq_len, seq_len), 1)
    is_valid = ((key_pos <= query_pos) & ((key_pos >= TEXT) | (key_pos < length)))[None]
    return (jnp.where(is_valid, scaled, -1e30), is_valid)


def attend_forward(inputs):
    query_rows, key_rows, value_rows, length = inputs
    masked, is_valid = masked_scores(query_rows, key_rows, length)
    row_top = jnp.max(masked, axis=-1, keepdims=True)
    exponent = jnp.where(is_valid, jnp.exp(ALPHA * (masked - row_top)), 0.0)
    row_total = jnp.sum(exponent, axis=-1, keepdims=True)
    weights_low = (exponent / row_total).astype(jnp.bfloat16)
    context = jnp.einsum(
        "hqk,khd->qhd", weights_low, value_rows, preferred_element_type=jnp.float32
    )
    return (context, row_top, row_total)


def attend_backward(inputs):
    query_rows, key_rows, value_rows, length, grad_context, row_top, row_total = inputs
    masked, is_valid = masked_scores(query_rows, key_rows, length)
    weights_soft = jnp.where(is_valid, jnp.exp(ALPHA * (masked - row_top)), 0.0) / row_total
    grad_values = jnp.einsum(
        "hqk,qhd->khd",
        weights_soft.astype(jnp.bfloat16),
        grad_context,
        preferred_element_type=jnp.float32,
    )
    grad_soft = jnp.einsum(
        "qhd,khd->hqk", grad_context, value_rows, preferred_element_type=jnp.float32
    )
    grad_expon = weights_soft * (
        grad_soft - jnp.sum(weights_soft * grad_soft, axis=-1, keepdims=True)
    )
    grad_scores = (grad_expon * ALPHA / (ALPHA * math.sqrt(HD))).astype(jnp.bfloat16)
    grad_queries = jnp.einsum(
        "hqk,khd->qhd", grad_scores, key_rows, preferred_element_type=jnp.float32
    )
    grad_keys = jnp.einsum(
        "hqk,qhd->khd", grad_scores, query_rows, preferred_element_type=jnp.float32
    )
    return (
        grad_queries.astype(jnp.bfloat16),
        grad_keys.astype(jnp.bfloat16),
        grad_values.astype(jnp.bfloat16),
    )


def local(
    tokens,
    text_lengths,
    norm1_gain,
    norm1_shift,
    w_qkv,
    q_bias,
    v_bias,
    w_out,
    out_bias,
    norm2_gain,
    norm2_shift,
    norm3_gain,
    norm3_shift,
    w_fc1,
    fc1_bias,
    w_fc2,
    fc2_bias,
    norm4_gain,
    norm4_shift,
    cotangent,
):
    seq_dev = text_lengths.shape[0]
    local_heads = q_bias.shape[0] // HD
    rows_all = seq_dev * LEN
    (gathered_first,) = segment(1, before_attention, [tokens], [norm1_gain, norm1_shift], [], 0)
    projected = jnp.dot(gathered_first, w_qkv, preferred_element_type=jnp.float32).reshape(
        rows_all, local_heads, 3, HD
    )
    seq_shape = (seq_dev, LEN, local_heads, HD)
    query_rows = (
        (projected[:, :, 0] + q_bias.reshape(local_heads, HD))
        .astype(jnp.bfloat16)
        .reshape(seq_shape)
    )
    key_rows = projected[:, :, 1].astype(jnp.bfloat16).reshape(seq_shape)
    value_rows = (
        (projected[:, :, 2] + v_bias.reshape(local_heads, HD))
        .astype(jnp.bfloat16)
        .reshape(seq_shape)
    )
    context, row_tops, row_totals = lax.map(
        attend_forward, (query_rows, key_rows, value_rows, text_lengths)
    )
    context_low = context.reshape(rows_all, local_heads * HD).astype(jnp.bfloat16)
    gathered_third, branch, hidden = segment(
        2, after_attention, [tokens],
        [out_bias, norm2_gain, norm2_shift, norm3_gain, norm3_shift],
        [jnp.float32, jnp.float32], 0, (context_low, w_out, False),
    )
    inner_act = jnp.dot(gathered_third, w_fc1, preferred_element_type=jnp.float32) + fc1_bias
    activated = jax.nn.gelu(inner_act, approximate=True).astype(LOW)
    gathered_grad, layer_out, sums4 = segment(
        3, turn_round, [hidden, cotangent], [fc2_bias, norm4_gain, norm4_shift],
        [LOW], 3, (activated, w_fc2, False),
    )
    grad_activated = times_transposed(gathered_grad, w_fc2)
    ffn_fc2 = transposed_times(activated, gathered_grad)
    grad_inner = gelu_back(inner_act, grad_activated).astype(LOW)
    ffn_fc1_bias = jnp.sum(grad_inner, axis=0, dtype=jnp.float32)
    ffn_fc1 = transposed_times(gathered_third, grad_inner)
    grad_inner, ffn_fc1, ffn_fc2 = lax.optimization_barrier(
        (grad_inner, ffn_fc1.astype(LOW), ffn_fc2.astype(LOW))
    )
    ffn_fc1, ffn_fc2 = lax.psum((ffn_fc1, ffn_fc2), "dp")
    gathered_branch, grad_hidden, sums3 = segment(
        4, after_feed_forward, [branch, hidden, cotangent],
        [norm2_gain, norm3_gain], [jnp.float32], 5, (grad_inner, w_fc1, True),
    )
    grad_context = times_transposed(gathered_branch, w_out).astype(jnp.bfloat16).reshape(seq_shape)
    part_out = transposed_times(context_low, gathered_branch)
    grad_queries, grad_keys, grad_values = lax.map(
        attend_backward,
        (query_rows, key_rows, value_rows, text_lengths, grad_context, row_tops, row_totals),
    )
    part_q_bias = jnp.sum(grad_queries, axis=(0, 1), dtype=jnp.float32).reshape(local_heads * HD)
    part_v_bias = jnp.sum(grad_values, axis=(0, 1), dtype=jnp.float32).reshape(local_heads * HD)
    grad_projected = jnp.stack([grad_queries, grad_keys, grad_values], axis=3).reshape(
        rows_all, 3 * local_heads * HD
    )
    part_qkv = transposed_times(gathered_first, grad_projected)
    width = w_out.shape[1]
    depth = w_out.shape[0]
    folded_out = part_out.astype(LOW).reshape(depth, width // depth, depth)
    folded_out = folded_out.transpose(1, 0, 2).reshape(width, depth)
    owned = jnp.concatenate([part_q_bias, part_v_bias, ffn_fc1_bias])
    input_grad, part_qkv, folded_out, shared, owned, _ = segment(
        5, at_the_input, [tokens, grad_hidden], [norm1_gain], [jnp.float32], 2,
        (grad_projected, w_qkv, True), False,
        (
            [part_qkv.astype(LOW), folded_out],
            jnp.concatenate([sums3, sums4]),
            owned.reshape(-1, width // lax.axis_size("tensor")),
        ),
    )
    part_out = folded_out.reshape(width // depth, depth, depth).transpose(1, 0, 2)
    part_out = part_out.reshape(depth, width)
    (
        grad_gain1,
        grad_shift1,
        grad_gain3,
        grad_shift3,
        grad_gain2,
        grad_shift2,
        grad_out_bias,
        grad_gain4,
        grad_shift4,
        grad_fc2_bias,
    ) = shared
    owned = owned.reshape(-1)
    cuts = [part_q_bias.shape[0], part_q_bias.shape[0] + part_v_bias.shape[0]]
    part_q_bias, part_v_bias, ffn_fc1_bias = jnp.split(owned, cuts)
    part_qkv, part_out, ffn_fc1, ffn_fc2 = (
        total.astype(jnp.float32) for total in (part_qkv, part_out, ffn_fc1, ffn_fc2)
    )
    return (
        layer_out,
        input_grad,
        grad_gain1,
        grad_shift1,
        part_qkv,
        part_q_bias,
        part_v_bias,
        part_out,
        grad_out_bias,
        grad_gain2,
        grad_shift2,
        grad_gain3,
        grad_shift3,
        ffn_fc1,
        ffn_fc1_bias,
        ffn_fc2,
        grad_fc2_bias,
        grad_gain4,
        grad_shift4,
    )


def solution(mesh):
    in_specs = (
        P(("dp", "tensor"), None),
        P("dp"),
        P(),
        P(),
        P(None, "tensor"),
        P("tensor"),
        P("tensor"),
        P("tensor", None),
        P(),
        P(),
        P(),
        P(),
        P(),
        P(None, "tensor"),
        P("tensor"),
        P("tensor", None),
        P(),
        P(),
        P(),
        P(("dp", "tensor"), None),
    )
    out_specs = (
        P(("dp", "tensor"), None),
        P(("dp", "tensor"), None),
        P(),
        P(),
        P(None, "tensor"),
        P("tensor"),
        P("tensor"),
        P("tensor", None),
        P(),
        P(),
        P(),
        P(),
        P(),
        P(None, "tensor"),
        P("tensor"),
        P("tensor", None),
        P(),
        P(),
        P(),
    )
    return jax.shard_map(
        local, mesh=mesh, in_specs=in_specs, out_specs=out_specs, check_vma=False
    )
```

```python
from functools import partial
import math

import jax
import jax.numpy as jnp
from jax import lax
from jax.experimental import pallas as pl
from jax.experimental.pallas import tpu as pltpu
from jax.sharding import PartitionSpec as P

HD = 64
TEXT = 64


epsilon = 1e-05


def times_transposed(left, right):
    return lax.dot_general(
        left, right, (((1,), (1,)), ((), ())), preferred_element_type=jnp.float32
    )


def transposed_times(left, right):
    return lax.dot_general(
        left, right, (((0,), (0,)), ((), ())), preferred_element_type=jnp.float32
    )


STEP = 64
TILE = 256
MESH = pl.DeviceIdType.MESH
LOW = jnp.bfloat16


def statistics(values):
    centered = values - jnp.mean(values, axis=-1, keepdims=True)
    inverse = lax.rsqrt(jnp.mean(centered * centered, axis=-1, keepdims=True) + epsilon)
    return centered * inverse, inverse


def norm_pullback(grad, normed, inverse, gain):
    scaled = grad * gain
    return inverse * (
        scaled
        - jnp.mean(scaled, axis=-1, keepdims=True)
        - normed * jnp.mean(scaled * normed, axis=-1, keepdims=True)
    )


def before_attention(total, rows, vectors):
    (token_rows,), (gain, shift) = rows, vectors
    normed, _ = statistics(token_rows)
    return normed * gain + shift, (), ()


def after_attention(total, rows, vectors):
    (token_rows,), (bias, gain2, shift2, gain3, shift3) = rows, vectors
    branch = total + bias
    normed, _ = statistics(branch)
    hidden = token_rows + (normed * gain2 + shift2)
    third, _ = statistics(hidden)
    return third * gain3 + shift3, (branch, hidden), ()


def turn_round(total, rows, vectors):
    (hidden, grad), (bias, gain, shift) = rows, vectors
    normed, inverse = statistics(total + bias)
    layer_out = hidden + (normed * gain + shift)
    low = norm_pullback(grad, normed, inverse, gain).astype(LOW).astype(jnp.float32)
    return low, (layer_out,), (grad * normed, grad, low)


def after_feed_forward(total, rows, vectors):
    (branch, hidden, grad), (gain2, gain3) = rows, vectors
    third, inverse3 = statistics(hidden)
    grad_hidden = grad + norm_pullback(total, third, inverse3, gain3)
    second, inverse2 = statistics(branch)
    low = norm_pullback(grad_hidden, second, inverse2, gain2).astype(LOW).astype(jnp.float32)
    return low, (grad_hidden,), (total * third, total, grad_hidden * second, grad_hidden, low)


def at_the_input(total, rows, vectors):
    (token_rows, grad_hidden), (gain,) = rows, vectors
    first, inverse = statistics(token_rows)
    return None, (grad_hidden + norm_pullback(total, first, inverse, gain),), (total * first, total)


class GroupSum:
    def __init__(self, sources, results, scratch):
        self.kept, self.near, self.far = scratch[:3]
        self.sems = scratch[3:]
        self.sources, self.results = sources, results
        self.pieces = [
            (at, column)
            for at, source in enumerate(sources)
            for column in range(0, source.shape[1], TILE)
        ]
        self.half = sources[0].shape[0] // 2
        self.peers = lax.axis_size("dp") // 2
        self.part = self.half // self.peers
        group = lax.axis_index("dp")
        self.side = lax.rem(group, 2)
        self.place = lax.div(group, 2)
        self.partner = group + 1 - 2 * self.side

    def others(self):
        for hop in range(1, self.peers):
            yield (
                hop - 1,
                lax.rem(self.place + hop, self.peers),
                lax.rem(self.place + self.peers - hop, self.peers),
            )

    def device(self, place):
        return place * 2 + self.side

    def targets(self):
        return [self.partner] + [self.device(ahead) for _, ahead, _ in self.others()]

    def send(self, source, target, outgoing, incoming, device):
        return pltpu.make_async_remote_copy(
            source, target, outgoing, incoming,
            device_id={"dp": device}, device_id_type=MESH,
        )

    def rows(self, start, size):
        return pl.ds(pl.multiple_of(start, 16), size)

    def cuts(self, piece):
        at, column = self.pieces[piece]
        return self.sources[at], self.results[at], pl.ds(column, TILE), pl.ds(piece * TILE, TILE)

    def halving(self, piece):
        source, _, cut, held = self.cuts(piece)
        return self.send(
            source.at[self.rows((1 - self.side) * self.half, self.half), cut],
            self.near.at[:, held], self.sems[0].at[piece], self.sems[1].at[piece], self.partner,
        )

    def parting(self, piece, slot, ahead):
        held = pl.ds(piece * TILE, TILE)
        return self.send(
            self.kept.at[self.rows(ahead * self.part, self.part), held], self.far.at[slot, :, held],
            self.sems[2].at[slot, piece], self.sems[3].at[slot, piece], self.device(ahead),
        )

    def joining(self, piece, slot, owner, ahead):
        _, result, cut, _ = self.cuts(piece)
        region = result.at[self.rows(self.side * self.half + owner * self.part, self.part), cut]
        return self.send(
            region, region, self.sems[4].at[slot, piece], self.sems[5].at[slot, piece],
            self.device(ahead),
        )

    def doubling(self, piece, side):
        _, result, cut, _ = self.cuts(piece)
        region = result.at[self.rows(side * self.half, self.half), cut]
        return self.send(
            region, region, self.sems[6].at[piece], self.sems[7].at[piece], self.partner
        )

    def start(self):
        for piece in range(len(self.pieces)):
            self.halving(piece).start()

    def after_halving(self, piece):
        source, _, cut, held = self.cuts(piece)
        self.halving(piece).wait_recv()
        mine = source[self.rows(self.side * self.half, self.half), cut].astype(jnp.float32)
        self.kept[:, held] = (mine + self.near[:, held].astype(jnp.float32)).astype(LOW)
        for slot, ahead, _ in self.others():
            self.parting(piece, slot, ahead).start()

    def after_parting(self, piece):
        _, result, cut, held = self.cuts(piece)
        total = self.kept[self.rows(self.place * self.part, self.part), held].astype(jnp.float32)
        for slot, ahead, _ in self.others():
            self.parting(piece, slot, ahead).wait_recv()
            total = total + self.far[slot, :, held].astype(jnp.float32)
        own = self.rows(self.side * self.half + self.place * self.part, self.part)
        result[own, cut] = total.astype(LOW)
        for slot, ahead, _ in self.others():
            self.joining(piece, slot, self.place, ahead).start()

    def after_joining(self, piece):
        for slot, ahead, behind in self.others():
            self.joining(piece, slot, behind, ahead).wait_recv()
        self.doubling(piece, self.side).start()

    def settle(self, piece):
        self.doubling(piece, 1 - self.side).wait_recv()
        self.doubling(piece, self.side).wait_send()
        self.halving(piece).wait_send()
        for slot, ahead, _ in self.others():
            self.parting(piece, slot, ahead).wait_send()
            self.joining(piece, slot, self.place, ahead).wait_send()


def group_sum_scratch(sources):
    pieces = sum(source.shape[1] for source in sources) // TILE
    half = sources[0].shape[0] // 2
    peers = lax.axis_size("dp") // 2
    width = pieces * TILE
    pair, fan = pltpu.SemaphoreType.DMA((pieces,)), pltpu.SemaphoreType.DMA((peers - 1, pieces))
    return [
        pltpu.VMEM((half, width), LOW),
        pltpu.VMEM((half, width), LOW),
        pltpu.VMEM((peers - 1, half // peers, width), LOW),
    ] + [pair, pair, fan, fan, fan, fan, pair, pair]


class SmallSum:
    def __init__(self, shared, owned, fresh, shared_out, owned_out, part, parts, turn, turns, last,
                 lasts, part_out, part_in, turn_out, turn_in, last_out, last_in):
        self.shared, self.owned, self.fresh = shared, owned, fresh
        self.shared_out, self.owned_out = shared_out, owned_out
        self.part, self.parts, self.turn, self.turns = part, parts, turn, turns
        self.last, self.lasts = last, lasts
        self.sems = part_out, part_in, turn_out, turn_in, last_out, last_in
        self.places, groups = lax.axis_size("tensor"), lax.axis_size("dp")
        self.groups = groups
        self.me, self.group = lax.axis_index("tensor"), lax.axis_index("dp")
        self.peers = [lax.rem(self.me + hop, self.places) for hop in range(1, self.places)]
        self.others = [lax.rem(self.group + hop, groups) for hop in range(1, groups)]
        self.n_fresh = fresh.shape[0]
        self.n_shared = self.n_fresh + shared.shape[0]
        self.quarter = shared.shape[-1] // self.places

    def sends(self, stage):
        axis = "dp" if stage == 1 else "tensor"
        outgoing, incoming = self.sems[2 * stage], self.sems[2 * stage + 1]
        for hop, peer in enumerate(self.others if stage == 1 else self.peers):
            if stage == 0:
                source, target = self.part.at[peer], self.parts.at[hop]
            elif stage == 1:
                source, target = self.turn, self.turns.at[self.group]
            else:
                source, target = self.last, self.lasts.at[self.me]
            yield pltpu.make_async_remote_copy(
                source, target, outgoing.at[hop], incoming.at[hop],
                device_id={axis: peer}, device_id_type=MESH,
            )

    def first_send(self):
        for place in range(self.places):
            cut = slice(place * self.quarter, (place + 1) * self.quarter)
            self.part[place, : self.n_fresh] = jnp.sum(self.fresh[:, :, cut], axis=1)
            self.part[place, self.n_fresh :] = jnp.sum(self.shared[:, :, cut], axis=1)
        for send in self.sends(0):
            send.start()

    def first_wait(self):
        total = self.part[self.me]
        for hop, send in enumerate(self.sends(0)):
            send.wait()
            total = total + self.parts[hop]
        self.turn[: self.n_shared] = total
        self.turn[self.n_shared :] = self.owned[...]
        self.turns[self.group] = self.turn[...]

    def second_send(self):
        for send in self.sends(1):
            send.start()

    def second_wait(self):
        for send in self.sends(1):
            send.wait()
        total = self.turns[0]
        for at in range(1, self.groups):
            total = total + self.turns[at]
        self.owned_out[...] = total[self.n_shared :]
        self.last[...] = total[: self.n_shared]
        self.lasts[self.me] = total[: self.n_shared]

    def third_send(self):
        for send in self.sends(2):
            send.start()

    def third_wait(self):
        for send in self.sends(2):
            send.wait()
        for place in range(self.places):
            cut = slice(place * self.quarter, (place + 1) * self.quarter)
            self.shared_out[:, cut] = self.lasts[place]


def small_sum_scratch(n_shared, owned):
    places, groups = lax.axis_size("tensor"), lax.axis_size("dp")
    quarter = owned.shape[1]
    depth = n_shared + owned.shape[0]
    return [
        pltpu.VMEM((places, n_shared, quarter), jnp.float32),
        pltpu.VMEM((places - 1, n_shared, quarter), jnp.float32),
        pltpu.VMEM((depth, quarter), jnp.float32),
        pltpu.VMEM((groups, depth, quarter), jnp.float32),
        pltpu.VMEM((n_shared, quarter), jnp.float32),
        pltpu.VMEM((places, n_shared, quarter), jnp.float32),
    ] + [
        pltpu.SemaphoreType.DMA((count,))
        for count in (places - 1, places - 1, groups - 1, groups - 1, places - 1, places - 1)
    ]


def segment_kernel(middle, counts, flipped, sending, *refs):
    n_rows, n_vectors, n_outs, n_sums, n_grouped = counts
    refs = list(refs)

    def take(count):
        taken = refs[:count]
        del refs[:count]
        return taken

    summing = flipped is not None
    if summing:
        left, right = take(2)
    row_refs, vector_refs = take(n_rows), take(n_vectors)
    if n_grouped:
        group_sources = take(n_grouped)
        small_in = take(2)
    gathered = take(1)[0] if sending else None
    out_refs = take(n_outs)
    if n_grouped:
        group_results = take(n_grouped)
        small_out = take(2)
    sums = take(1)[0] if n_sums else None
    if summing:
        give, got, keep, onward, came, give_sem, got_sem, out_sem, in_sem = take(9)
    if sending:
        near_out, near_in, far_out, far_in, on_out, on_in = take(6)
    if n_grouped:
        grouped = GroupSum(group_sources, group_results, take(11))
        small = SmallSum(*small_in, sums, *small_out, *take(12))

    me = lax.axis_index("tensor")
    partner = me + 1 - 2 * lax.rem(me, 2)
    across = lax.rem(me + 2, 4)
    diagonal = 3 - me
    share, width = row_refs[0].shape
    whole = share // STEP
    rest = share - whole * STEP

    def each(body):
        def one(at, carry):
            body(at, pl.multiple_of(at * STEP, STEP), STEP)
            return carry

        lax.fori_loop(0, whole, one, 0)
        if rest:
            body(whole, whole * STEP, rest)

    barrier = pltpu.get_barrier_semaphore()
    for peer in (partner, across):
        pl.semaphore_signal(barrier, inc=1, device_id={"tensor": peer}, device_id_type=MESH)
    if n_grouped:
        pl.semaphore_signal(
            barrier, inc=1, device_id={"tensor": diagonal}, device_id_type=MESH
        )
        for other in small.others:
            pl.semaphore_signal(barrier, inc=1, device_id={"dp": other}, device_id_type=MESH)
        pl.semaphore_wait(barrier, 3 + len(small.others))
        grouped.start()
    else:
        pl.semaphore_wait(barrier, 2)

    def product(block, target):
        rows = pl.ds(pl.multiple_of(block * share, 16), share)

        def one(at, carry):
            cut = pl.ds(pl.multiple_of(at * TILE, TILE), TILE)
            if flipped:
                value = times_transposed(left[rows, :], right[cut, :])
            else:
                value = jnp.dot(left[rows, :], right[:, cut], preferred_element_type=jnp.float32)
            target[:, cut] = value.astype(target.dtype)
            return carry

        lax.fori_loop(0, width // TILE, one, 0)

    if summing:

        def gift(at):
            return pltpu.make_async_remote_copy(
                give.at[at], got.at[at], give_sem.at[at], got_sem.at[at],
                device_id={"tensor": partner}, device_id_type=MESH,
            )

        def crossing(at, start, size):
            cut = pl.ds(start, size)
            return pltpu.make_async_remote_copy(
                onward.at[cut], came.at[cut], out_sem.at[at], in_sem.at[at],
                device_id={"tensor": across}, device_id_type=MESH,
            )

        product(diagonal, give.at[0])
        product(across, keep.at[0])
        gift(0).start()
        product(partner, give.at[1])
        gift(0).wait_recv()

        def pass_on(at, start, size):
            cut = pl.ds(start, size)
            onward[cut] = (keep[0, cut] + got[0, cut].astype(jnp.float32)).astype(LOW)
            crossing(at, start, size).start()

        each(pass_on)
        gift(1).start()
        product(me, keep.at[1])
        gift(1).wait_recv()

    if n_sums:
        sums[...] = jnp.zeros_like(sums)
    vectors = [ref[...] for ref in vector_refs]

    def spread(target, block, sems, at, start, size):
        cut = pl.ds(pl.multiple_of(block * share + start, 16), size)
        return pltpu.make_async_remote_copy(
            gathered.at[cut], gathered.at[cut], sems[0].at[at], sems[1].at[at],
            device_id={"tensor": target}, device_id_type=MESH,
        )

    def finish(at, start, size):
        cut = pl.ds(start, size)
        total = None
        if summing:
            crossing(at, start, size).wait_recv()
            total = (
                keep[1, cut] + got[1, cut].astype(jnp.float32) + came[cut].astype(jnp.float32)
            )
        result, outs, terms = middle(
            total, [ref[cut].astype(jnp.float32) for ref in row_refs], vectors
        )
        if sending:
            own = pl.ds(pl.multiple_of(me * share + start, 16), size)
            gathered[own] = result.astype(LOW)
        for ref, value in zip(out_refs, outs):
            ref[cut] = value.astype(ref.dtype)
        for index, term in enumerate(terms):
            sums[index] += jnp.sum(term.reshape(size // 8, 8, width), axis=0)
        if sending:
            spread(across, me, (far_out, far_in), at, start, size).start()
            spread(partner, me, (near_out, near_in), at, start, size).start()

    if n_grouped:
        pieces = len(grouped.pieces)
        early = pieces // 2
        for piece in range(early):
            grouped.after_halving(piece)
        each(finish)
        small.first_send()
        for piece in range(early, pieces):
            grouped.after_halving(piece)
            grouped.after_parting(piece - early)
        small.first_wait()
        small.second_send()
        for piece in range(pieces - early, pieces):
            grouped.after_joining(piece - (pieces - early))
            grouped.after_parting(piece)
        small.second_wait()
        small.third_send()
        for piece in range(early, pieces):
            grouped.after_joining(piece)
        small.third_wait()
        for piece in range(pieces):
            grouped.settle(piece)
    else:
        each(finish)

    if sending:

        def relay(at, start, size):
            spread(across, across, (far_out, far_in), at, start, size).wait_recv()
            spread(partner, across, (on_out, on_in), at, start, size).start()

        def settle(at, start, size):
            spread(partner, partner, (near_out, near_in), at, start, size).wait()
            spread(across, me, (far_out, far_in), at, start, size).wait_send()
            spread(partner, diagonal, (on_out, on_in), at, start, size).wait()

        each(relay)
        each(settle)
    if summing:
        gift(0).wait_send()
        gift(1).wait_send()
        each(lambda at, start, size: crossing(at, start, size).wait_send())


def segment(number, middle, rows, vectors, outs, n_sums, product=None, sending=True,
            grouped=None):
    share, width = rows[0].shape
    flipped = None
    operands = []
    shapes = []
    scratch = []
    pieces = -(-share // STEP)
    places = lax.axis_size("tensor")
    flops = 0
    if product is not None:
        left, right, flipped = product
        operands += [left, right]
        flops = 2 * left.shape[0] * right.size
        scratch += [
            pltpu.VMEM((2, share, width), LOW),
            pltpu.VMEM((2, share, width), LOW),
            pltpu.VMEM((2, share, width), jnp.float32),
            pltpu.VMEM((share, width), LOW),
            pltpu.VMEM((share, width), LOW),
            pltpu.SemaphoreType.DMA((2,)),
            pltpu.SemaphoreType.DMA((2,)),
            pltpu.SemaphoreType.DMA((pieces,)),
            pltpu.SemaphoreType.DMA((pieces,)),
        ]
    operands += list(rows) + [vector.reshape(1, width) for vector in vectors]
    n_grouped = 0
    if grouped is not None:
        sources, small_shared, small_owned = grouped
        n_grouped = len(sources)
        n_shared = n_sums + small_shared.shape[0]
        operands += list(sources) + [small_shared, small_owned]
    if sending:
        shapes.append(jax.ShapeDtypeStruct((places * share, width), LOW))
        scratch += [pltpu.SemaphoreType.DMA((pieces,))] * 6
    shapes += [jax.ShapeDtypeStruct((share, width), dtype) for dtype in outs]
    if n_grouped:
        shapes += [jax.ShapeDtypeStruct(source.shape, LOW) for source in sources]
        shapes.append(jax.ShapeDtypeStruct((n_shared, width), jnp.float32))
        shapes.append(jax.ShapeDtypeStruct(small_owned.shape, jnp.float32))
        scratch += group_sum_scratch(sources) + small_sum_scratch(n_shared, small_owned)
    if n_sums:
        shapes.append(jax.ShapeDtypeStruct((n_sums, 8, width), jnp.float32))
    counts = (len(rows), len(vectors), len(outs), n_sums, n_grouped)
    in_vmem = pl.BlockSpec(memory_space=pltpu.VMEM)
    moved = sum(item.size * item.dtype.itemsize for item in operands + shapes)
    return pl.pallas_call(
        partial(segment_kernel, middle, counts, flipped, sending),
        out_shape=shapes,
        in_specs=[in_vmem] * len(operands),
        out_specs=[in_vmem] * len(shapes),
        scratch_shapes=scratch,
        compiler_params=pltpu.CompilerParams(
            collective_id=number, has_side_effects=True, vmem_limit_bytes=48 * 2**20
        ),
        cost_estimate=pl.CostEstimate(
            flops=flops + 25_000_000_000, bytes_accessed=moved, transcendentals=0
        ),
    )(*operands)


def gelu_back(inner_act, grad_act):
    _, pullback = jax.vjp(partial(jax.nn.gelu, approximate=True), inner_act)
    return pullback(grad_act)[0]


QUERIES = 256
FIRST = 128
PAIR = 2
SCALE = 1.0 / math.sqrt(HD)


def blocks_of(rows):
    return [(start, min(QUERIES, rows - start)) for start in range(0, rows, QUERIES)]


def key_pieces(start, size):
    if start == 0:
        return [(0, size, True, True)]
    pieces = [(0, FIRST, False, True)]
    if start > FIRST:
        pieces.append((FIRST, start, False, False))
    return pieces + [(start, start + size, True, False)]


def hide(values, key_axis, keys_from, queries_from, causal, first, length, hidden):
    if not (causal or first):
        return values
    keys = keys_from + lax.broadcasted_iota(jnp.int32, values.shape, key_axis)
    valid = None
    if causal:
        queries = queries_from + lax.broadcasted_iota(jnp.int32, values.shape, 1 - key_axis)
        valid = keys <= queries
    if first:
        real = (keys >= TEXT) | (keys < length)
        valid = real if valid is None else valid & real
    return jnp.where(valid, values, hidden)


def part_of(packed, head, part):
    start = (head * 3 + part) * HD
    return packed[:, start : start + HD]


def attend_kernel(lengths, packed_ref, context_ref, top_ref):
    length = lengths[pl.program_id(0)]
    packed = packed_ref[...]
    outs = []
    for head in range(PAIR):
        queries = part_of(packed, head, 0) * jnp.bfloat16(SCALE)
        keys, values = part_of(packed, head, 1), part_of(packed, head, 2)
        contexts = []
        for start, size in blocks_of(packed.shape[0]):
            mine = queries[start : start + size]
            pieces = key_pieces(start, size)
            scores = [
                hide(times_transposed(mine, keys[low:high]), 1, low, start, causal, first,
                     length, -1e30)
                for low, high, causal, first in pieces
            ]
            top = scores[0].max(axis=1, keepdims=True)
            for score in scores[1:]:
                top = jnp.maximum(top, score.max(axis=1, keepdims=True))
            raised = [jnp.exp(score - top) for score in scores]
            total = sum(part.sum(axis=1, keepdims=True) for part in raised)
            inverse = 1.0 / total
            context = sum(
                jnp.dot((part * inverse).astype(LOW), values[low:high],
                        preferred_element_type=jnp.float32)
                for part, (low, high, _, _) in zip(raised, pieces)
            )
            contexts.append(context)
            top_ref[0, 0, start : start + size, head : head + 1] = top + jnp.log(total)
        outs.append(jnp.concatenate(contexts, axis=0))
    context_ref[...] = jnp.concatenate(outs, axis=1).astype(LOW)


def attend_back_kernel(lengths, packed_ref, grad_ref, top_ref, out_ref, column_ref, *scratch):
    length = lengths[pl.program_id(0)]
    packed = packed_ref[...]
    grads = grad_ref[...]
    outs = []
    for head in range(PAIR):
        grad_keys, grad_values, grad_queries = scratch[3 * head : 3 * head + 3]
        queries = part_of(packed, head, 0) * jnp.bfloat16(SCALE)
        keys, values = part_of(packed, head, 1), part_of(packed, head, 2)
        grad = grads[:, head * HD : (head + 1) * HD]
        grad_keys[...] = jnp.zeros_like(grad_keys)
        grad_values[...] = jnp.zeros_like(grad_values)
        for start, size in blocks_of(packed.shape[0]):
            mine, grad_mine = queries[start : start + size], grad[start : start + size]
            top = top_ref[0, 0, head : head + 1, start : start + size]
            pieces = key_pieces(start, size)
            weights, products = [], []
            for low, high, causal, first in pieces:
                score = times_transposed(keys[low:high], mine)
                weight = jnp.exp(
                    hide(score, 0, low, start, causal, first, length, -1e30) - top
                )
                weights.append(weight)
                grad_values[low:high] += jnp.dot(
                    weight.astype(LOW), grad_mine, preferred_element_type=jnp.float32
                )
                products.append(times_transposed(values[low:high], grad_mine))
            mean = sum(
                (weight * product).sum(axis=0, keepdims=True)
                for weight, product in zip(weights, products)
            )
            turned = 0.0
            for (low, high, _, _), weight, product in zip(pieces, weights, products):
                grad_score = (weight * (product - mean)).astype(LOW)
                grad_keys[low:high] += jnp.dot(
                    grad_score, mine, preferred_element_type=jnp.float32
                )
                turned = turned + transposed_times(keys[low:high], grad_score)
            grad_queries[start : start + size] = turned.T * SCALE
        outs += [grad_queries[...], grad_keys[...], grad_values[...]]
    packed_grad = jnp.concatenate(outs, axis=1).astype(LOW)
    out_ref[...] = packed_grad
    column_ref[0, 0] = jnp.sum(packed_grad.astype(jnp.float32), axis=0, keepdims=True)


def attend(packed, lengths):
    sequences = lengths.shape[0]
    rows = packed.shape[0] // sequences
    pairs = packed.shape[1] // (3 * PAIR * HD)
    area = packed.shape[0] * rows * pairs * PAIR
    return pl.pallas_call(
        attend_kernel,
        grid=(sequences, pairs),
        in_specs=[
            pl.BlockSpec(memory_space=pltpu.SMEM),
            pl.BlockSpec((rows, 3 * PAIR * HD), lambda at, pair: (at, pair)),
        ],
        out_specs=[
            pl.BlockSpec((rows, PAIR * HD), lambda at, pair: (at, pair)),
            pl.BlockSpec((1, 1, rows, PAIR), lambda at, pair: (at, pair, 0, 0)),
        ],
        out_shape=[
            jax.ShapeDtypeStruct((packed.shape[0], pairs * PAIR * HD), LOW),
            jax.ShapeDtypeStruct((sequences, pairs, rows, PAIR), jnp.float32),
        ],
        cost_estimate=pl.CostEstimate(
            flops=8 * area * HD, bytes_accessed=3 * packed.size, transcendentals=area
        ),
        name="attend",
    )(lengths, packed)


def attend_back(packed, grad_context, tops, lengths):
    sequences = lengths.shape[0]
    rows = packed.shape[0] // sequences
    pairs = packed.shape[1] // (3 * PAIR * HD)
    area = packed.shape[0] * rows * pairs * PAIR
    return pl.pallas_call(
        attend_back_kernel,
        grid=(sequences, pairs),
        in_specs=[
            pl.BlockSpec(memory_space=pltpu.SMEM),
            pl.BlockSpec((rows, 3 * PAIR * HD), lambda at, pair: (at, pair)),
            pl.BlockSpec((rows, PAIR * HD), lambda at, pair: (at, pair)),
            pl.BlockSpec((1, 1, PAIR, rows), lambda at, pair: (at, pair, 0, 0)),
        ],
        out_specs=[
            pl.BlockSpec((rows, 3 * PAIR * HD), lambda at, pair: (at, pair)),
            pl.BlockSpec((1, 1, 1, 3 * PAIR * HD), lambda at, pair: (at, pair, 0, 0)),
        ],
        out_shape=[
            jax.ShapeDtypeStruct(packed.shape, LOW),
            jax.ShapeDtypeStruct((sequences, pairs, 1, 3 * PAIR * HD), jnp.float32),
        ],
        scratch_shapes=[pltpu.VMEM((rows, HD), jnp.float32)] * (3 * PAIR),
        cost_estimate=pl.CostEstimate(
            flops=20 * area * HD, bytes_accessed=5 * packed.size, transcendentals=area
        ),
        name="attend_back",
    )(lengths, packed, grad_context, tops)


def local(
    tokens,
    text_lengths,
    norm1_gain,
    norm1_shift,
    w_qkv,
    q_bias,
    v_bias,
    w_out,
    out_bias,
    norm2_gain,
    norm2_shift,
    norm3_gain,
    norm3_shift,
    w_fc1,
    fc1_bias,
    w_fc2,
    fc2_bias,
    norm4_gain,
    norm4_shift,
    cotangent,
):
    local_heads = q_bias.shape[0] // HD
    (gathered_first,) = segment(1, before_attention, [tokens], [norm1_gain, norm1_shift], [], 0)
    biases = jnp.stack(
        [q_bias.reshape(-1, HD), jnp.zeros((local_heads, HD)), v_bias.reshape(-1, HD)], axis=1
    ).reshape(1, -1)
    packed = (
        jnp.dot(gathered_first, w_qkv, preferred_element_type=jnp.float32) + biases
    ).astype(LOW)
    context_low, tops = attend(packed, text_lengths)
    gathered_third, branch, hidden = segment(
        2, after_attention, [tokens],
        [out_bias, norm2_gain, norm2_shift, norm3_gain, norm3_shift],
        [jnp.float32, jnp.float32], 0, (context_low, w_out, False),
    )
    inner_act = jnp.dot(gathered_third, w_fc1, preferred_element_type=jnp.float32) + fc1_bias
    activated = jax.nn.gelu(inner_act, approximate=True).astype(LOW)
    gathered_grad, layer_out, sums4 = segment(
        3, turn_round, [hidden, cotangent], [fc2_bias, norm4_gain, norm4_shift],
        [LOW], 3, (activated, w_fc2, False),
    )
    grad_activated = times_transposed(gathered_grad, w_fc2)
    ffn_fc2 = transposed_times(activated, gathered_grad)
    grad_inner = gelu_back(inner_act, grad_activated).astype(LOW)
    ffn_fc1_bias = jnp.sum(grad_inner, axis=0, dtype=jnp.float32)
    ffn_fc1 = transposed_times(gathered_third, grad_inner)
    grad_inner, ffn_fc1, ffn_fc2 = lax.optimization_barrier(
        (grad_inner, ffn_fc1.astype(LOW), ffn_fc2.astype(LOW))
    )
    ffn_fc1, ffn_fc2 = lax.psum((ffn_fc1, ffn_fc2), "dp")
    gathered_branch, grad_hidden, sums3 = segment(
        4, after_feed_forward, [branch, hidden, cotangent],
        [norm2_gain, norm3_gain], [jnp.float32], 5, (grad_inner, w_fc1, True),
    )
    grad_context = times_transposed(gathered_branch, w_out).astype(LOW)
    part_out = transposed_times(context_low, gathered_branch)
    grad_projected, columns = attend_back(
        packed, grad_context, tops.transpose(0, 1, 3, 2), text_lengths
    )
    columns = columns.sum(axis=0).reshape(local_heads, 3, HD)
    part_q_bias, part_v_bias = columns[:, 0].reshape(-1), columns[:, 2].reshape(-1)
    part_qkv = transposed_times(gathered_first, grad_projected)
    width = w_out.shape[1]
    depth = w_out.shape[0]
    folded_out = part_out.astype(LOW).reshape(depth, width // depth, depth)
    folded_out = folded_out.transpose(1, 0, 2).reshape(width, depth)
    owned = jnp.concatenate([part_q_bias, part_v_bias, ffn_fc1_bias])
    input_grad, part_qkv, folded_out, shared, owned, _ = segment(
        5, at_the_input, [tokens, grad_hidden], [norm1_gain], [jnp.float32], 2,
        (grad_projected, w_qkv, True), False,
        (
            [part_qkv.astype(LOW), folded_out],
            jnp.concatenate([sums3, sums4]),
            owned.reshape(-1, width // lax.axis_size("tensor")),
        ),
    )
    part_out = folded_out.reshape(width // depth, depth, depth).transpose(1, 0, 2)
    part_out = part_out.reshape(depth, width)
    (
        grad_gain1,
        grad_shift1,
        grad_gain3,
        grad_shift3,
        grad_gain2,
        grad_shift2,
        grad_out_bias,
        grad_gain4,
        grad_shift4,
        grad_fc2_bias,
    ) = shared
    owned = owned.reshape(-1)
    cuts = [part_q_bias.shape[0], part_q_bias.shape[0] + part_v_bias.shape[0]]
    part_q_bias, part_v_bias, ffn_fc1_bias = jnp.split(owned, cuts)
    part_qkv, part_out, ffn_fc1, ffn_fc2 = (
        total.astype(jnp.float32) for total in (part_qkv, part_out, ffn_fc1, ffn_fc2)
    )
    return (
        layer_out,
        input_grad,
        grad_gain1,
        grad_shift1,
        part_qkv,
        part_q_bias,
        part_v_bias,
        part_out,
        grad_out_bias,
        grad_gain2,
        grad_shift2,
        grad_gain3,
        grad_shift3,
        ffn_fc1,
        ffn_fc1_bias,
        ffn_fc2,
        grad_fc2_bias,
        grad_gain4,
        grad_shift4,
    )


def solution(mesh):
    in_specs = (
        P(("dp", "tensor"), None),
        P("dp"),
        P(),
        P(),
        P(None, "tensor"),
        P("tensor"),
        P("tensor"),
        P("tensor", None),
        P(),
        P(),
        P(),
        P(),
        P(),
        P(None, "tensor"),
        P("tensor"),
        P("tensor", None),
        P(),
        P(),
        P(),
        P(("dp", "tensor"), None),
    )
    out_specs = (
        P(("dp", "tensor"), None),
        P(("dp", "tensor"), None),
        P(),
        P(),
        P(None, "tensor"),
        P("tensor"),
        P("tensor"),
        P("tensor", None),
        P(),
        P(),
        P(),
        P(),
        P(),
        P(None, "tensor"),
        P("tensor"),
        P("tensor", None),
        P(),
        P(),
        P(),
    )
    return jax.shard_map(
        local, mesh=mesh, in_specs=in_specs, out_specs=out_specs, check_vma=False
    )
```

```python
from functools import partial
import math

import jax
import jax.numpy as jnp
from jax import lax
from jax.experimental import pallas as pl
from jax.experimental.pallas import tpu as pltpu
from jax.sharding import PartitionSpec as P

HD = 64
TEXT = 64


epsilon = 1e-05


def times_transposed(left, right):
    return lax.dot_general(
        left, right, (((1,), (1,)), ((), ())), preferred_element_type=jnp.float32
    )


def transposed_times(left, right):
    return lax.dot_general(
        left, right, (((0,), (0,)), ((), ())), preferred_element_type=jnp.float32
    )


STEP = 64
TILE = 256
FINISH_AT = 14.0
MESH = pl.DeviceIdType.MESH
LOW = jnp.bfloat16


def statistics(values):
    centered = values - jnp.mean(values, axis=-1, keepdims=True)
    inverse = lax.rsqrt(jnp.mean(centered * centered, axis=-1, keepdims=True) + epsilon)
    return centered * inverse, inverse


def norm_pullback(grad, normed, inverse, gain):
    scaled = grad * gain
    return inverse * (
        scaled
        - jnp.mean(scaled, axis=-1, keepdims=True)
        - normed * jnp.mean(scaled * normed, axis=-1, keepdims=True)
    )


def before_attention(total, rows, vectors):
    (token_rows,), (gain, shift) = rows, vectors
    normed, _ = statistics(token_rows)
    return normed * gain + shift, (), ()


def after_attention(total, rows, vectors):
    (token_rows,), (bias, gain2, shift2, gain3, shift3) = rows, vectors
    branch = total + bias
    normed, _ = statistics(branch)
    hidden = token_rows + (normed * gain2 + shift2)
    third, _ = statistics(hidden)
    return third * gain3 + shift3, (branch, hidden), ()


def turn_round(total, rows, vectors):
    (hidden, grad), (bias, gain, shift) = rows, vectors
    normed, inverse = statistics(total + bias)
    layer_out = hidden + (normed * gain + shift)
    low = norm_pullback(grad, normed, inverse, gain).astype(LOW).astype(jnp.float32)
    return low, (layer_out,), (grad * normed, grad, low)


def after_feed_forward(total, rows, vectors):
    (branch, hidden, grad), (gain2, gain3) = rows, vectors
    third, inverse3 = statistics(hidden)
    grad_hidden = grad + norm_pullback(total, third, inverse3, gain3)
    second, inverse2 = statistics(branch)
    low = norm_pullback(grad_hidden, second, inverse2, gain2).astype(LOW).astype(jnp.float32)
    return low, (grad_hidden,), (total * third, total, grad_hidden * second, grad_hidden, low)


def at_the_input(total, rows, vectors):
    (token_rows, grad_hidden), (gain,) = rows, vectors
    first, inverse = statistics(token_rows)
    return None, (grad_hidden + norm_pullback(total, first, inverse, gain),), (total * first, total)


class GroupSum:
    def __init__(self, sources, results, scratch, scatter=True, gather=True):
        self.scatter, self.gather = scatter, gather
        scratch = list(scratch)
        if scatter:
            self.kept, self.fresh, self.half_out, self.half_in = scratch[:4]
            scratch = scratch[4:]
        if gather:
            self.join_out, self.join_in = scratch
        self.sources, self.results = sources, results
        groups = lax.axis_size("dp")
        self.stages = groups.bit_length() - 1
        self.depth = sources[0].shape[0] if scatter else results[0].shape[0]
        self.pieces = [
            (at, column)
            for at, source in enumerate(sources)
            for column in range(0, source.shape[1], TILE)
        ]
        self.group = lax.axis_index("dp")
        self.routes = [self.route() for _ in range(len(self.pieces))]

    def partner(self, bit):
        side = lax.rem(lax.div(self.group, 2**bit), 2)
        return side, self.group + (1 - 2 * side) * 2**bit

    def route(self):
        bits = list(range(self.stages))
        start, size, route = 0, self.depth, []
        for bit in bits:
            side, partner = self.partner(bit)
            size //= 2
            route.append((partner, start + side * size, start + (1 - side) * size, size))
            start = start + side * size
        return route

    def rows(self, start, size):
        return pl.ds(pl.multiple_of(start, 16), size)

    def cuts(self, piece):
        at, column = self.pieces[piece]
        return self.sources[at], self.results[at], pl.ds(column, TILE), pl.ds(piece * TILE, TILE)

    def halving(self, piece, stage):
        source, _, cut, held = self.cuts(piece)
        partner, _, given, size = self.routes[piece][stage]
        given = self.rows(given, size)
        return pltpu.make_async_remote_copy(
            self.kept.at[given, held] if stage else source.at[given, cut],
            self.fresh.at[pl.ds(self.depth - 2 * size, size), held],
            self.half_out.at[stage, piece], self.half_in.at[stage, piece],
            device_id={"dp": partner}, device_id_type=MESH,
        )

    def joining(self, piece, stage, arriving=False):
        source, result, cut, _ = self.cuts(piece)
        partner, kept, given, size = self.routes[piece][stage]
        region = result.at[self.rows(given if arriving else kept, size), cut]
        first = stage == self.stages - 1 and not self.scatter
        return pltpu.make_async_remote_copy(
            source.at[:, cut] if first else region, region,
            self.join_out.at[stage, piece], self.join_in.at[stage, piece],
            device_id={"dp": partner}, device_id_type=MESH,
        )

    def start(self):
        for piece in range(len(self.pieces)):
            self.halving(piece, 0).start()

    def start_joining(self):
        for piece in range(len(self.pieces)):
            self.joining(piece, self.stages - 1).start()
        for piece in range(len(self.pieces)):
            source, result, cut, _ = self.cuts(piece)
            _, kept, _, size = self.routes[piece][-1]
            result[self.rows(kept, size), cut] = source[:, cut]

    def after_halving(self, piece, stage):
        source, result, cut, held = self.cuts(piece)
        _, kept, _, size = self.routes[piece][stage]
        own = self.rows(kept, size)
        self.halving(piece, stage).wait_recv()
        mine = self.kept[own, held] if stage else source[own, cut]
        arrived = self.fresh[pl.ds(self.depth - 2 * size, size), held]
        total = (mine.astype(jnp.float32) + arrived.astype(jnp.float32)).astype(LOW)
        if stage + 1 < self.stages:
            self.kept[own, held] = total
            self.halving(piece, stage + 1).start()
        elif self.gather:
            result[own, cut] = total
            self.joining(piece, stage).start()
        else:
            result[:, cut] = total

    def after_joining(self, piece, stage):
        self.joining(piece, stage, True).wait_recv()
        if stage:
            self.joining(piece, stage - 1).start()

    def settle(self):
        for piece in range(len(self.pieces)):
            for stage in range(self.stages):
                if self.scatter:
                    self.halving(piece, stage).wait_send()
                if self.gather:
                    self.joining(piece, stage).wait_send()

    def scatter_steps(self, pace, hop, begin=0.0):
        for piece in range(len(self.pieces)):
            for stage in range(self.stages):
                when = begin + pace * (piece + 1) + hop * stage
                yield when, partial(self.after_halving, piece, stage)

    def gather_steps(self, pace, hop, begin=0.0):
        for piece in range(len(self.pieces)):
            for stage in range(self.stages):
                late = 0.0 if stage else 1000.0
                when = begin + late + pace * (piece + 1) + hop * (self.stages - 1 - stage)
                yield when, partial(self.after_joining, piece, stage)


def in_turn(steps):
    for _, step in sorted(steps, key=lambda item: item[0]):
        step()


def group_sum_scratch(sources, scatter=True, gather=True):
    pieces = sum(source.shape[1] for source in sources) // TILE
    depth = sources[0].shape[0]
    width = pieces * TILE
    sems = pltpu.SemaphoreType.DMA((lax.axis_size("dp").bit_length() - 1, pieces))
    held = [pltpu.VMEM((depth, width), LOW), pltpu.VMEM((depth, width), LOW), sems, sems]
    return (held if scatter else []) + ([sems, sems] if gather else [])


class SmallSum:
    def __init__(self, shared, owned, fresh, shared_out, owned_out, part, parts, turn, turns, last,
                 lasts, part_out, part_in, turn_out, turn_in, last_out, last_in):
        self.shared, self.owned, self.fresh = shared, owned, fresh
        self.shared_out, self.owned_out = shared_out, owned_out
        self.part, self.parts, self.turn, self.turns = part, parts, turn, turns
        self.last, self.lasts = last, lasts
        self.sems = part_out, part_in, turn_out, turn_in, last_out, last_in
        self.places, groups = lax.axis_size("tensor"), lax.axis_size("dp")
        self.groups = groups
        self.me, self.group = lax.axis_index("tensor"), lax.axis_index("dp")
        self.peers = [lax.rem(self.me + hop, self.places) for hop in range(1, self.places)]
        self.others = [lax.rem(self.group + hop, groups) for hop in range(1, groups)]
        self.n_fresh = fresh.shape[0]
        self.n_shared = self.n_fresh + shared.shape[0]
        self.quarter = shared.shape[-1] // self.places

    def sends(self, stage):
        axis = "dp" if stage == 1 else "tensor"
        outgoing, incoming = self.sems[2 * stage], self.sems[2 * stage + 1]
        for hop, peer in enumerate(self.others if stage == 1 else self.peers):
            if stage == 0:
                source, target = self.part.at[peer], self.parts.at[hop]
            elif stage == 1:
                source, target = self.turn, self.turns.at[self.group]
            else:
                source, target = self.last, self.lasts.at[self.me]
            yield pltpu.make_async_remote_copy(
                source, target, outgoing.at[hop], incoming.at[hop],
                device_id={axis: peer}, device_id_type=MESH,
            )

    def first_send(self):
        for place in range(self.places):
            cut = slice(place * self.quarter, (place + 1) * self.quarter)
            self.part[place, : self.n_fresh] = jnp.sum(self.fresh[:, :, cut], axis=1)
            self.part[place, self.n_fresh :] = jnp.sum(self.shared[:, :, cut], axis=1)
        for send in self.sends(0):
            send.start()

    def first_wait(self):
        total = self.part[self.me]
        for hop, send in enumerate(self.sends(0)):
            send.wait()
            total = total + self.parts[hop]
        self.turn[: self.n_shared] = total
        self.turn[self.n_shared :] = self.owned[...]
        self.turns[self.group] = self.turn[...]

    def second_send(self):
        for send in self.sends(1):
            send.start()

    def second_wait(self):
        for send in self.sends(1):
            send.wait()
        total = self.turns[0]
        for at in range(1, self.groups):
            total = total + self.turns[at]
        self.owned_out[...] = total[self.n_shared :]
        self.last[...] = total[: self.n_shared]
        self.lasts[self.me] = total[: self.n_shared]

    def third_send(self):
        for send in self.sends(2):
            send.start()

    def third_wait(self):
        for send in self.sends(2):
            send.wait()
        for place in range(self.places):
            cut = slice(place * self.quarter, (place + 1) * self.quarter)
            self.shared_out[:, cut] = self.lasts[place]


def small_sum_scratch(n_shared, owned):
    places, groups = lax.axis_size("tensor"), lax.axis_size("dp")
    quarter = owned.shape[1]
    depth = n_shared + owned.shape[0]
    return [
        pltpu.VMEM((places, n_shared, quarter), jnp.float32),
        pltpu.VMEM((places - 1, n_shared, quarter), jnp.float32),
        pltpu.VMEM((depth, quarter), jnp.float32),
        pltpu.VMEM((groups, depth, quarter), jnp.float32),
        pltpu.VMEM((n_shared, quarter), jnp.float32),
        pltpu.VMEM((places, n_shared, quarter), jnp.float32),
    ] + [
        pltpu.SemaphoreType.DMA((count,))
        for count in (places - 1, places - 1, groups - 1, groups - 1, places - 1, places - 1)
    ]


def segment_kernel(middle, counts, flipped, sending, *refs):
    n_rows, n_vectors, n_outs, n_sums, n_grouped, n_parted, n_joined = counts
    refs = list(refs)

    def take(count):
        taken = refs[:count]
        del refs[:count]
        return taken

    summing = flipped is not None
    if summing:
        left, right = take(2)
    row_refs, vector_refs = take(n_rows), take(n_vectors)
    if n_grouped:
        group_sources = take(n_grouped)
        small_in = take(2)
        joined_sources = take(n_joined)
    if n_parted:
        group_sources = take(n_parted)
    gathered = take(1)[0] if sending else None
    out_refs = take(n_outs)
    if n_grouped:
        group_results = take(n_grouped)
        small_out = take(2)
        joined_results = take(n_joined)
    if n_parted:
        group_results = take(n_parted)
    sums = take(1)[0] if n_sums else None
    if summing:
        give, got, keep, onward, came, give_sem, got_sem, out_sem, in_sem = take(9)
    if sending:
        near_out, near_in, far_out, far_in, on_out, on_in = take(6)
    if n_grouped:
        grouped = GroupSum(group_sources, group_results, take(6))
        small = SmallSum(*small_in, sums, *small_out, *take(12))
        joined = GroupSum(joined_sources, joined_results, take(2), False, True)
    if n_parted:
        grouped = GroupSum(group_sources, group_results, take(4), True, False)

    me = lax.axis_index("tensor")
    partner = me + 1 - 2 * lax.rem(me, 2)
    across = lax.rem(me + 2, 4)
    diagonal = 3 - me
    share, width = row_refs[0].shape
    whole = share // STEP
    rest = share - whole * STEP

    def each(body):
        def one(at, carry):
            body(at, pl.multiple_of(at * STEP, STEP), STEP)
            return carry

        lax.fori_loop(0, whole, one, 0)
        if rest:
            body(whole, whole * STEP, rest)

    barrier = pltpu.get_barrier_semaphore()
    for peer in (partner, across):
        pl.semaphore_signal(barrier, inc=1, device_id={"tensor": peer}, device_id_type=MESH)
    if n_grouped:
        pl.semaphore_signal(
            barrier, inc=1, device_id={"tensor": diagonal}, device_id_type=MESH
        )
        for other in small.others:
            pl.semaphore_signal(barrier, inc=1, device_id={"dp": other}, device_id_type=MESH)
        pl.semaphore_wait(barrier, 3 + len(small.others))
        grouped.start()
        joined.start_joining()
    elif n_parted:
        for bit in range(grouped.stages):
            _, other = grouped.partner(bit)
            pl.semaphore_signal(barrier, inc=1, device_id={"dp": other}, device_id_type=MESH)
        pl.semaphore_wait(barrier, 2 + grouped.stages)
        grouped.start()
    else:
        pl.semaphore_wait(barrier, 2)

    def product(block, target):
        rows = pl.ds(pl.multiple_of(block * share, 16), share)

        def one(at, carry):
            cut = pl.ds(pl.multiple_of(at * TILE, TILE), TILE)
            if flipped:
                value = times_transposed(left[rows, :], right[cut, :])
            else:
                value = jnp.dot(left[rows, :], right[:, cut], preferred_element_type=jnp.float32)
            target[:, cut] = value.astype(target.dtype)
            return carry

        lax.fori_loop(0, width // TILE, one, 0)

    if summing:

        def gift(at):
            return pltpu.make_async_remote_copy(
                give.at[at], got.at[at], give_sem.at[at], got_sem.at[at],
                device_id={"tensor": partner}, device_id_type=MESH,
            )

        def crossing(at, start, size):
            cut = pl.ds(start, size)
            return pltpu.make_async_remote_copy(
                onward.at[cut], came.at[cut], out_sem.at[at], in_sem.at[at],
                device_id={"tensor": across}, device_id_type=MESH,
            )

        product(diagonal, give.at[0])
        product(across, keep.at[0])
        gift(0).start()
        product(partner, give.at[1])
        gift(0).wait_recv()

        def pass_on(at, start, size):
            cut = pl.ds(start, size)
            onward[cut] = (keep[0, cut] + got[0, cut].astype(jnp.float32)).astype(LOW)
            crossing(at, start, size).start()

        each(pass_on)
        gift(1).start()
        product(me, keep.at[1])
        gift(1).wait_recv()

    if n_sums:
        sums[...] = jnp.zeros_like(sums)
    vectors = [ref[...] for ref in vector_refs]

    def spread(target, block, sems, at, start, size):
        cut = pl.ds(pl.multiple_of(block * share + start, 16), size)
        return pltpu.make_async_remote_copy(
            gathered.at[cut], gathered.at[cut], sems[0].at[at], sems[1].at[at],
            device_id={"tensor": target}, device_id_type=MESH,
        )

    def finish(at, start, size):
        cut = pl.ds(start, size)
        total = None
        if summing:
            crossing(at, start, size).wait_recv()
            total = (
                keep[1, cut] + got[1, cut].astype(jnp.float32) + came[cut].astype(jnp.float32)
            )
        result, outs, terms = middle(
            total, [ref[cut].astype(jnp.float32) for ref in row_refs], vectors
        )
        if sending:
            own = pl.ds(pl.multiple_of(me * share + start, 16), size)
            gathered[own] = result.astype(LOW)
        for ref, value in zip(out_refs, outs):
            ref[cut] = value.astype(ref.dtype)
        for index, term in enumerate(terms):
            sums[index] += jnp.sum(term.reshape(size // 8, 8, width), axis=0)
        if sending:
            spread(across, me, (far_out, far_in), at, start, size).start()
            spread(partner, me, (near_out, near_in), at, start, size).start()

    steps = [(FINISH_AT, partial(each, finish))]
    if n_grouped:
        steps += list(grouped.scatter_steps(6.0, 12.0))
        steps += list(grouped.gather_steps(6.0, 6.0, 36.0))
        steps += list(joined.gather_steps(4.0, 4.0))
        steps += [
            (FINISH_AT + 0.5, small.first_send),
            (FINISH_AT + 8, small.first_wait),
            (FINISH_AT + 8, small.second_send),
            (FINISH_AT + 30, small.second_wait),
            (FINISH_AT + 30, small.third_send),
            (1000.0, small.third_wait),
            (2000.0, grouped.settle),
            (2000.0, joined.settle),
        ]
    elif n_parted:
        steps += list(grouped.scatter_steps(6.0, 5.0))
        steps.append((2000.0, grouped.settle))

    if sending:

        def relay(at, start, size):
            spread(across, across, (far_out, far_in), at, start, size).wait_recv()
            spread(partner, across, (on_out, on_in), at, start, size).start()

        def settle(at, start, size):
            spread(partner, partner, (near_out, near_in), at, start, size).wait()
            spread(across, me, (far_out, far_in), at, start, size).wait_send()
            spread(partner, diagonal, (on_out, on_in), at, start, size).wait()

        steps += [(FINISH_AT + 14, partial(each, relay)), (1500.0, partial(each, settle))]
    in_turn(steps)
    if summing:
        gift(0).wait_send()
        gift(1).wait_send()
        each(lambda at, start, size: crossing(at, start, size).wait_send())


def segment(number, middle, rows, vectors, outs, n_sums, product=None, sending=True,
            grouped=None, parted=()):
    share, width = rows[0].shape
    flipped = None
    operands = []
    shapes = []
    scratch = []
    pieces = -(-share // STEP)
    places = lax.axis_size("tensor")
    flops = 0
    if product is not None:
        left, right, flipped = product
        operands += [left, right]
        flops = 2 * left.shape[0] * right.size
        scratch += [
            pltpu.VMEM((2, share, width), LOW),
            pltpu.VMEM((2, share, width), LOW),
            pltpu.VMEM((2, share, width), jnp.float32),
            pltpu.VMEM((share, width), LOW),
            pltpu.VMEM((share, width), LOW),
            pltpu.SemaphoreType.DMA((2,)),
            pltpu.SemaphoreType.DMA((2,)),
            pltpu.SemaphoreType.DMA((pieces,)),
            pltpu.SemaphoreType.DMA((pieces,)),
        ]
    operands += list(rows) + [vector.reshape(1, width) for vector in vectors]
    n_grouped = n_joined = 0
    if grouped is not None:
        sources, small_shared, small_owned, joined = grouped
        n_joined = len(joined)
        n_grouped = len(sources)
        n_shared = n_sums + small_shared.shape[0]
        operands += list(sources) + [small_shared, small_owned] + list(joined)
    n_parted = len(parted)
    operands += list(parted)
    if sending:
        shapes.append(jax.ShapeDtypeStruct((places * share, width), LOW))
        scratch += [pltpu.SemaphoreType.DMA((pieces,))] * 6
    shapes += [jax.ShapeDtypeStruct((share, width), dtype) for dtype in outs]
    if n_grouped:
        shapes += [jax.ShapeDtypeStruct(source.shape, LOW) for source in sources]
        shapes.append(jax.ShapeDtypeStruct((n_shared, width), jnp.float32))
        shapes.append(jax.ShapeDtypeStruct(small_owned.shape, jnp.float32))
        groups = lax.axis_size("dp")
        shapes += [
            jax.ShapeDtypeStruct((item.shape[0] * groups, item.shape[1]), LOW) for item in joined
        ]
        scratch += group_sum_scratch(sources) + small_sum_scratch(n_shared, small_owned)
        scratch += group_sum_scratch(joined, False, True)
    if n_parted:
        groups = lax.axis_size("dp")
        shapes += [
            jax.ShapeDtypeStruct((item.shape[0] // groups, item.shape[1]), LOW) for item in parted
        ]
        scratch += group_sum_scratch(parted, True, False)
    if n_sums:
        shapes.append(jax.ShapeDtypeStruct((n_sums, 8, width), jnp.float32))
    counts = (len(rows), len(vectors), len(outs), n_sums, n_grouped, n_parted, n_joined)
    in_vmem = pl.BlockSpec(memory_space=pltpu.VMEM)
    moved = sum(item.size * item.dtype.itemsize for item in operands + shapes)
    return pl.pallas_call(
        partial(segment_kernel, middle, counts, flipped, sending),
        out_shape=shapes,
        in_specs=[in_vmem] * len(operands),
        out_specs=[in_vmem] * len(shapes),
        scratch_shapes=scratch,
        compiler_params=pltpu.CompilerParams(
            collective_id=number, has_side_effects=True, vmem_limit_bytes=48 * 2**20
        ),
        cost_estimate=pl.CostEstimate(
            flops=flops + 25_000_000_000, bytes_accessed=moved, transcendentals=0
        ),
    )(*operands)


def gelu_back(inner_act, grad_act):
    _, pullback = jax.vjp(partial(jax.nn.gelu, approximate=True), inner_act)
    return pullback(grad_act)[0]


QUERIES = 256
FIRST = 128
PAIR = 2
SCALE = 1.0 / math.sqrt(HD)


def blocks_of(rows):
    return [(start, min(QUERIES, rows - start)) for start in range(0, rows, QUERIES)]


def key_pieces(start, size):
    if start == 0:
        return [(0, size, True, True)]
    pieces = [(0, FIRST, False, True)]
    if start > FIRST:
        pieces.append((FIRST, start, False, False))
    return pieces + [(start, start + size, True, False)]


def hide(values, key_axis, keys_from, queries_from, causal, first, length, hidden):
    if not (causal or first):
        return values
    keys = keys_from + lax.broadcasted_iota(jnp.int32, values.shape, key_axis)
    valid = None
    if causal:
        queries = queries_from + lax.broadcasted_iota(jnp.int32, values.shape, 1 - key_axis)
        valid = keys <= queries
    if first:
        real = (keys >= TEXT) | (keys < length)
        valid = real if valid is None else valid & real
    return jnp.where(valid, values, hidden)


def part_of(packed, head, part):
    start = (head * 3 + part) * HD
    return packed[:, start : start + HD]


def attend_kernel(lengths, packed_ref, context_ref, top_ref):
    length = lengths[pl.program_id(0)]
    packed = packed_ref[...]
    outs = []
    for head in range(PAIR):
        queries = part_of(packed, head, 0) * jnp.bfloat16(SCALE)
        keys, values = part_of(packed, head, 1), part_of(packed, head, 2)
        contexts = []
        for start, size in blocks_of(packed.shape[0]):
            mine = queries[start : start + size]
            pieces = key_pieces(start, size)
            scores = [
                hide(times_transposed(mine, keys[low:high]), 1, low, start, causal, first,
                     length, -1e30)
                for low, high, causal, first in pieces
            ]
            top = scores[0].max(axis=1, keepdims=True)
            for score in scores[1:]:
                top = jnp.maximum(top, score.max(axis=1, keepdims=True))
            raised = [jnp.exp(score - top) for score in scores]
            total = sum(part.sum(axis=1, keepdims=True) for part in raised)
            inverse = 1.0 / total
            context = sum(
                jnp.dot((part * inverse).astype(LOW), values[low:high],
                        preferred_element_type=jnp.float32)
                for part, (low, high, _, _) in zip(raised, pieces)
            )
            contexts.append(context)
            top_ref[0, 0, start : start + size, head : head + 1] = top + jnp.log(total)
        outs.append(jnp.concatenate(contexts, axis=0))
    context_ref[...] = jnp.concatenate(outs, axis=1).astype(LOW)


def attend_back_kernel(lengths, packed_ref, grad_ref, top_ref, out_ref, column_ref, *scratch):
    length = lengths[pl.program_id(0)]
    packed = packed_ref[...]
    grads = grad_ref[...]
    outs = []
    for head in range(PAIR):
        grad_keys, grad_values, grad_queries = scratch[3 * head : 3 * head + 3]
        queries = part_of(packed, head, 0) * jnp.bfloat16(SCALE)
        keys, values = part_of(packed, head, 1), part_of(packed, head, 2)
        grad = grads[:, head * HD : (head + 1) * HD]
        grad_keys[...] = jnp.zeros_like(grad_keys)
        grad_values[...] = jnp.zeros_like(grad_values)
        for start, size in blocks_of(packed.shape[0]):
            mine, grad_mine = queries[start : start + size], grad[start : start + size]
            top = top_ref[0, 0, head : head + 1, start : start + size]
            pieces = key_pieces(start, size)
            weights, products = [], []
            for low, high, causal, first in pieces:
                score = times_transposed(keys[low:high], mine)
                weight = jnp.exp(
                    hide(score, 0, low, start, causal, first, length, -1e30) - top
                )
                weights.append(weight)
                grad_values[low:high] += jnp.dot(
                    weight.astype(LOW), grad_mine, preferred_element_type=jnp.float32
                )
                products.append(times_transposed(values[low:high], grad_mine))
            mean = sum(
                (weight * product).sum(axis=0, keepdims=True)
                for weight, product in zip(weights, products)
            )
            turned = 0.0
            for (low, high, _, _), weight, product in zip(pieces, weights, products):
                grad_score = (weight * (product - mean)).astype(LOW)
                grad_keys[low:high] += jnp.dot(
                    grad_score, mine, preferred_element_type=jnp.float32
                )
                turned = turned + transposed_times(keys[low:high], grad_score)
            grad_queries[start : start + size] = turned.T * SCALE
        outs += [grad_queries[...], grad_keys[...], grad_values[...]]
    packed_grad = jnp.concatenate(outs, axis=1).astype(LOW)
    out_ref[...] = packed_grad
    column_ref[0, 0] = jnp.sum(packed_grad.astype(jnp.float32), axis=0, keepdims=True)


def attend(packed, lengths):
    sequences = lengths.shape[0]
    rows = packed.shape[0] // sequences
    pairs = packed.shape[1] // (3 * PAIR * HD)
    area = packed.shape[0] * rows * pairs * PAIR
    return pl.pallas_call(
        attend_kernel,
        grid=(sequences, pairs),
        in_specs=[
            pl.BlockSpec(memory_space=pltpu.SMEM),
            pl.BlockSpec((rows, 3 * PAIR * HD), lambda at, pair: (at, pair)),
        ],
        out_specs=[
            pl.BlockSpec((rows, PAIR * HD), lambda at, pair: (at, pair)),
            pl.BlockSpec((1, 1, rows, PAIR), lambda at, pair: (at, pair, 0, 0)),
        ],
        out_shape=[
            jax.ShapeDtypeStruct((packed.shape[0], pairs * PAIR * HD), LOW),
            jax.ShapeDtypeStruct((sequences, pairs, rows, PAIR), jnp.float32),
        ],
        cost_estimate=pl.CostEstimate(
            flops=8 * area * HD, bytes_accessed=3 * packed.size, transcendentals=area
        ),
        name="attend",
    )(lengths, packed)


def attend_back(packed, grad_context, tops, lengths):
    sequences = lengths.shape[0]
    rows = packed.shape[0] // sequences
    pairs = packed.shape[1] // (3 * PAIR * HD)
    area = packed.shape[0] * rows * pairs * PAIR
    return pl.pallas_call(
        attend_back_kernel,
        grid=(sequences, pairs),
        in_specs=[
            pl.BlockSpec(memory_space=pltpu.SMEM),
            pl.BlockSpec((rows, 3 * PAIR * HD), lambda at, pair: (at, pair)),
            pl.BlockSpec((rows, PAIR * HD), lambda at, pair: (at, pair)),
            pl.BlockSpec((1, 1, PAIR, rows), lambda at, pair: (at, pair, 0, 0)),
        ],
        out_specs=[
            pl.BlockSpec((rows, 3 * PAIR * HD), lambda at, pair: (at, pair)),
            pl.BlockSpec((1, 1, 1, 3 * PAIR * HD), lambda at, pair: (at, pair, 0, 0)),
        ],
        out_shape=[
            jax.ShapeDtypeStruct(packed.shape, LOW),
            jax.ShapeDtypeStruct((sequences, pairs, 1, 3 * PAIR * HD), jnp.float32),
        ],
        scratch_shapes=[pltpu.VMEM((rows, HD), jnp.float32)] * (3 * PAIR),
        cost_estimate=pl.CostEstimate(
            flops=20 * area * HD, bytes_accessed=5 * packed.size, transcendentals=area
        ),
        name="attend_back",
    )(lengths, packed, grad_context, tops)


def local(
    tokens,
    text_lengths,
    norm1_gain,
    norm1_shift,
    w_qkv,
    q_bias,
    v_bias,
    w_out,
    out_bias,
    norm2_gain,
    norm2_shift,
    norm3_gain,
    norm3_shift,
    w_fc1,
    fc1_bias,
    w_fc2,
    fc2_bias,
    norm4_gain,
    norm4_shift,
    cotangent,
):
    local_heads = q_bias.shape[0] // HD
    (gathered_first,) = segment(1, before_attention, [tokens], [norm1_gain, norm1_shift], [], 0)
    biases = jnp.stack(
        [q_bias.reshape(-1, HD), jnp.zeros((local_heads, HD)), v_bias.reshape(-1, HD)], axis=1
    ).reshape(1, -1)
    packed = (
        jnp.dot(gathered_first, w_qkv, preferred_element_type=jnp.float32) + biases
    ).astype(LOW)
    context_low, tops = attend(packed, text_lengths)
    gathered_third, branch, hidden = segment(
        2, after_attention, [tokens],
        [out_bias, norm2_gain, norm2_shift, norm3_gain, norm3_shift],
        [jnp.float32, jnp.float32], 0, (context_low, w_out, False),
    )
    inner_act = jnp.dot(gathered_third, w_fc1, preferred_element_type=jnp.float32) + fc1_bias
    activated = jax.nn.gelu(inner_act, approximate=True).astype(LOW)
    gathered_grad, layer_out, sums4 = segment(
        3, turn_round, [hidden, cotangent], [fc2_bias, norm4_gain, norm4_shift],
        [LOW], 3, (activated, w_fc2, False),
    )
    ffn_fc2 = transposed_times(activated, gathered_grad).astype(LOW)
    gathered_grad, ffn_fc2 = lax.optimization_barrier((gathered_grad, ffn_fc2))
    ffn_fc2 = lax.psum(ffn_fc2, "dp")
    grad_activated = times_transposed(gathered_grad, w_fc2)
    grad_inner = gelu_back(inner_act, grad_activated).astype(LOW)
    ffn_fc1_bias = jnp.sum(grad_inner, axis=0, dtype=jnp.float32)
    ffn_fc1 = transposed_times(gathered_third, grad_inner).astype(LOW)
    gathered_branch, grad_hidden, ffn_fc1, sums3 = segment(
        4, after_feed_forward, [branch, hidden, cotangent],
        [norm2_gain, norm3_gain], [jnp.float32], 5, (grad_inner, w_fc1, True), True, None,
        [ffn_fc1],
    )
    grad_context = times_transposed(gathered_branch, w_out).astype(LOW)
    part_out = transposed_times(context_low, gathered_branch)
    grad_projected, columns = attend_back(
        packed, grad_context, tops.transpose(0, 1, 3, 2), text_lengths
    )
    columns = columns.sum(axis=0).reshape(local_heads, 3, HD)
    part_q_bias, part_v_bias = columns[:, 0].reshape(-1), columns[:, 2].reshape(-1)
    part_qkv = transposed_times(gathered_first, grad_projected)
    width = w_out.shape[1]
    depth = w_out.shape[0]
    folded_out = part_out.astype(LOW).reshape(depth, width // depth, depth)
    folded_out = folded_out.transpose(1, 0, 2).reshape(width, depth)
    owned = jnp.concatenate([part_q_bias, part_v_bias, ffn_fc1_bias])
    input_grad, part_qkv, folded_out, shared, owned, ffn_fc1, _ = segment(
        5, at_the_input, [tokens, grad_hidden], [norm1_gain], [jnp.float32], 2,
        (grad_projected, w_qkv, True), False,
        (
            [part_qkv.astype(LOW), folded_out],
            jnp.concatenate([sums3, sums4]),
            owned.reshape(-1, width // lax.axis_size("tensor")),
            [ffn_fc1],
        ),
    )
    part_out = folded_out.reshape(width // depth, depth, depth).transpose(1, 0, 2)
    part_out = part_out.reshape(depth, width)
    (
        grad_gain1,
        grad_shift1,
        grad_gain3,
        grad_shift3,
        grad_gain2,
        grad_shift2,
        grad_out_bias,
        grad_gain4,
        grad_shift4,
        grad_fc2_bias,
    ) = shared
    owned = owned.reshape(-1)
    cuts = [part_q_bias.shape[0], part_q_bias.shape[0] + part_v_bias.shape[0]]
    part_q_bias, part_v_bias, ffn_fc1_bias = jnp.split(owned, cuts)
    part_qkv, part_out, ffn_fc1, ffn_fc2 = (
        total.astype(jnp.float32) for total in (part_qkv, part_out, ffn_fc1, ffn_fc2)
    )
    return (
        layer_out,
        input_grad,
        grad_gain1,
        grad_shift1,
        part_qkv,
        part_q_bias,
        part_v_bias,
        part_out,
        grad_out_bias,
        grad_gain2,
        grad_shift2,
        grad_gain3,
        grad_shift3,
        ffn_fc1,
        ffn_fc1_bias,
        ffn_fc2,
        grad_fc2_bias,
        grad_gain4,
        grad_shift4,
    )


def solution(mesh):
    in_specs = (
        P(("dp", "tensor"), None),
        P("dp"),
        P(),
        P(),
        P(None, "tensor"),
        P("tensor"),
        P("tensor"),
        P("tensor", None),
        P(),
        P(),
        P(),
        P(),
        P(),
        P(None, "tensor"),
        P("tensor"),
        P("tensor", None),
        P(),
        P(),
        P(),
        P(("dp", "tensor"), None),
    )
    out_specs = (
        P(("dp", "tensor"), None),
        P(("dp", "tensor"), None),
        P(),
        P(),
        P(None, "tensor"),
        P("tensor"),
        P("tensor"),
        P("tensor", None),
        P(),
        P(),
        P(),
        P(),
        P(),
        P(None, "tensor"),
        P("tensor"),
        P("tensor", None),
        P(),
        P(),
        P(),
    )
    return jax.shard_map(
        local, mesh=mesh, in_specs=in_specs, out_specs=out_specs, check_vma=False
    )
```
